128 devices in a mesh: bx: 16 (over x, z_lo, core), by: 8 (over z_hi, y).
Axes of the slice: x: 4, y: 4, z: 4 (z_hi: 2, z_lo: 2; z = z_hi * 2 + z_lo), core: 2. Of those that a mesh axis runs over, the one named last changes fastest.
Arguments:
- photon_data: float32 [6, 1024, 256, 128], P(None, 'bx', 'by'), may hold values from 0 to 1, as said below
- block_counts: int32 [1024, 256], P('bx', 'by'), may hold values from 1 to 128
- gather_offsets: float32 [3, 524288], P(None, ('bx', 'by')), may hold values from 0 to 1, as said below
- gather_blocks: int32 [4, 524288], P(None, ('bx', 'by')), may hold values from 0 to 262143, as said below
- albedo: float32 [3, 524288], P(None, ('bx', 'by')), may hold values from 0.1 to 1
- gather_pixels: int32 [524288], P(('bx', 'by')), may hold values from 0 to 262143, as said below
- tile_slot: int32 [1024], replicated, may hold values from 0 to 1023, as said below
Outputs:
- film: float32 [3, 1024, 256], P(None, ('bx', 'by'))
The draws below stay inside these ranges and needn't reach their ends.
Inputs may be any that keep to these rules, and one draw needn't show every extreme that they name: `photon_data`: per point and channel in cell units: entries 0 to 2 are a position in [0, 1), entries 3 to 5 a positive power. `gather_offsets`: each coordinate lies in [0, 1). `gather_blocks`: entry 0 is the point's own cell, inside the brick of the device that holds the point; the 4 entries are the four different cells of a 2 x 2 square of cells (periodic) that contains it. `gather_pixels`: in the rows of one device, at most 96 gather points lie in tiles whose slots s share s // 8; in every draw some such owner group receives exactly 96 from every device. `tile_slot`: A permutation of 0 to 1023.
All inputs are finite; a program needn't handle non-finite values.
Results may differ from the reference program's by a relative error of at most 0.0003.
Values sent between devices are 32-bit elements; how exact they have to be, the bound alone decides.
No kernel may reach another device: no remote copies, remote signals or barrier semaphores. Data moves between devices by JAX's collectives and lax.ppermute only.
A program may use at most 512 MiB of HBM per device.

```python
import math
import jax
import jax.numpy as jnp
from jax import lax

CX = 64
CY = 32
SLOTS = 128
LISTED = 4
G_DEV = 4096
TILE_PIX = 256
TILE_DEV = 8
OWNERS = 128
NXC = 1024
NYC = 256
NG = 524288
TILES = 1024
CAP = 96


def gather_geometry(key):
    base = jax.random.fold_in(key, 11)
    keys = jax.random.split(base, 5)
    rows = jnp.arange(NG, dtype=jnp.int32)
    device = rows // G_DEV
    bricks_y = NYC // CY
    home_x = device // bricks_y * CX + jax.random.randint(keys[0], (NG,), 0, CX)
    home_y = device % bricks_y * CY + jax.random.randint(keys[1], (NG,), 0, CY)
    step_x = 2 * jax.random.randint(keys[2], (NG,), 0, 2) - 1
    step_y = 2 * jax.random.randint(keys[3], (NG,), 0, 2) - 1
    turn = jax.random.randint(keys[4], (NG,), 0, 3)
    return (home_x, home_y, step_x, step_y, turn)


def owner_plan(key):
    base = jax.random.fold_in(key, 23)
    keys = jax.random.split(base, 5)
    perm = jax.random.permutation(keys[0], TILES).astype(jnp.int32)
    pool = OWNERS * CAP
    heavy = jax.random.randint(keys[1], (), 0, OWNERS)
    owner_of = jnp.arange(pool, dtype=jnp.int32) // CAP

    def one_device(dev_key):
        scores = jax.random.permutation(dev_key, pool).astype(jnp.int32)
        order = jnp.argsort(jnp.where(owner_of == heavy, 0, pool) + scores, stable=True)
        picked = order[:G_DEV] // CAP
        mixing = jax.random.permutation(jax.random.fold_in(dev_key, 1), G_DEV)
        return picked[mixing].astype(jnp.int32)
    dev_keys = jax.vmap(lambda d: jax.random.fold_in(keys[2], d))(jnp.arange(OWNERS))
    owner = jax.vmap(one_device)(dev_keys).reshape(NG)
    local_tile = jax.random.randint(keys[3], (NG,), 0, TILE_DEV)
    slot = owner * TILE_DEV + local_tile
    inverse = jnp.argsort(perm, stable=True).astype(jnp.int32)
    tile = inverse[slot]
    pixel = tile * TILE_PIX + jax.random.randint(keys[4], (NG,), 0, TILE_PIX)
    return (perm, pixel.astype(jnp.int32))


def draw_tile_slot(key, part):
    return owner_plan(key)[0]


def draw_gather_pixels(key, part):
    return owner_plan(key)[1]


def draw_gather_blocks(key, part):
    home_x, home_y, step_x, step_y, turn = gather_geometry(key)
    own = home_x * NYC + home_y
    beside_x = (home_x + step_x) % NXC * NYC + home_y
    beside_y = home_x * NYC + (home_y + step_y) % NYC
    beside_xy = (home_x + step_x) % NXC * NYC + (home_y + step_y) % NYC
    others = jnp.stack([beside_x, beside_y, beside_xy])
    picks = []
    for entry in range(3):
        which = (entry + turn) % 3
        picks.append(jnp.where(which == 0, others[0], jnp.where(which == 1, others[1], others[2])))
    return jnp.stack([own] + picks).astype(jnp.int32)


def draw_gather_offsets(key, part):
    home_x, home_y, step_x, step_y, turn = gather_geometry(key)
    uniforms = jax.random.uniform(jax.random.fold_in(key, 12), (3, NG), jnp.float32, 0.0, 0.999)
    off_x = jnp.where(step_x > 0, 0.5 + 0.49 * uniforms[0], 0.5 - 0.5 * uniforms[0])
    off_y = jnp.where(step_y > 0, 0.5 + 0.49 * uniforms[1], 0.5 - 0.5 * uniforms[1])
    return jnp.stack([off_x, off_y, uniforms[2]]).astype(jnp.float32)


def draw_photon_data(key, part):
    keys = jax.random.split(jax.random.fold_in(key, 31), 2)
    places = jax.random.uniform(keys[0], (3, NXC, NYC, SLOTS), jnp.float32, 0.0, 0.999)
    log_power = jax.random.uniform(keys[1], (3, NXC, NYC, SLOTS), jnp.float32, jnp.log(0.02), jnp.log(0.2))
    power = jnp.exp(log_power)
    return jnp.concatenate([places, power], axis=0).astype(jnp.float32)


def place_ends(result, rng, smallest, largest):
    longest = result.shape.index(max(result.shape))
    spots = []
    for shift in (0, 1):
        where = [jax.random.randint(jax.random.fold_in(rng, axis), (), 0, length) for axis, length in enumerate(result.shape)]
        where[longest] = (where[longest] + shift) % result.shape[longest]
        spots.append(tuple(where))
    return result.at[spots[0]].set(smallest).at[spots[1]].set(largest)


def block_scale(own_key, dims, cuts, low, largest):
    factor_of, own = 1.0, jax.random.fold_in(own_key, 6)
    for position, blocks in cuts:
        draws = jnp.exp(jax.random.uniform(jax.random.fold_in(own, position), (blocks,), jnp.float32, low / len(cuts), largest / len(cuts)))
        factor_of = factor_of * jnp.repeat(draws, dims[position] // blocks).reshape([-1 if axis == position else 1 for axis in range(len(dims))])
    return factor_of


def setup_inputs(seed: int = 0) -> dict:
    splits = jax.random.split(jax.random.key(seed), 8)
    return {
        "photon_data": draw_photon_data(jax.random.fold_in(splits[7], 71), 0),
        "block_counts": place_ends(jax.random.randint(splits[1], (NXC, NYC), 1, SLOTS + 1), jax.random.fold_in(splits[1], 1), 1, SLOTS).astype(jnp.int32),
        "gather_offsets": draw_gather_offsets(jax.random.fold_in(splits[7], 71), 0),
        "gather_blocks": draw_gather_blocks(jax.random.fold_in(splits[7], 71), 0),
        "albedo": jnp.clip(jnp.exp(math.log(1.0) - 2.3025851 * jax.random.uniform(splits[4], (3, NG), jnp.float32) ** block_scale(splits[4], (3, NG), ((1, 128),), -0.2, 0.2)), 0.1, 1.0),
        "gather_pixels": draw_gather_pixels(jax.random.fold_in(splits[7], 71), 0),
        "tile_slot": draw_tile_slot(jax.random.fold_in(splits[7], 71), 0),
    }


RADIUS_SQ = 0.25


def kernel_sum(blocks, live, shift_x, shift_y, offsets, albedo):
    delta_x = (shift_x[:, :, None] + blocks[0]) - offsets[0][:, None, None]
    delta_y = (shift_y[:, :, None] + blocks[1]) - offsets[1][:, None, None]
    delta_z = blocks[2] - offsets[2][:, None, None]
    dist_sq = delta_x * delta_x + delta_y * delta_y + delta_z * delta_z
    weight = jnp.maximum(1.0 - dist_sq / RADIUS_SQ, 0.0)
    weight = jnp.where(live, weight, 0.0)
    sums = jnp.sum(weight[None] * blocks[3:6], axis=(2, 3))
    return albedo * sums


def reference(photon_data, block_counts, gather_offsets, gather_blocks, albedo, gather_pixels, tile_slot):
    slots = photon_data.shape[3]
    table = photon_data.reshape(6, NXC * NYC, slots)
    count_table = block_counts.reshape(NXC * NYC)
    group = math.gcd(NG, 4096)
    groups = NG // group
    ids = gather_blocks.reshape(LISTED, groups, group).transpose(1, 2, 0)
    offs = gather_offsets.reshape(3, groups, group).transpose(1, 0, 2)
    albs = albedo.reshape(3, groups, group).transpose(1, 0, 2)

    def one_group(packed):
        idb, off, alb = packed
        cell_x = idb // NYC
        cell_y = idb % NYC
        shift_x = ((cell_x - cell_x[:, :1] + 1) % NXC - 1).astype(jnp.float32)
        shift_y = ((cell_y - cell_y[:, :1] + 1) % NYC - 1).astype(jnp.float32)
        flat = idb.reshape(-1)
        blocks = jnp.take(table, flat, axis=1).reshape(6, group, LISTED, slots)
        counts = jnp.take(count_table, flat).reshape(group, LISTED)
        live = jnp.arange(slots, dtype=jnp.int32)[None, None, :] < counts[:, :, None]
        return kernel_sum(blocks, live, shift_x, shift_y, off, alb)

    rad = lax.map(one_group, (ids, offs, albs))
    radiance = rad.transpose(1, 0, 2).reshape(3, NG)
    tile = gather_pixels // TILE_PIX
    slot = jnp.take(tile_slot, tile)
    target = slot * TILE_PIX + gather_pixels % TILE_PIX
    film = jnp.zeros((3, TILES * TILE_PIX), jnp.float32).at[:, target].add(radiance)
    return film.reshape(3, TILES, TILE_PIX)
```

```python
import jax
import jax.numpy as jnp
from jax import lax
from jax.experimental import pallas as pl
from jax.experimental.pallas import tpu as pltpu
from jax.sharding import PartitionSpec as P

AXES = ("bx", "by")
CX, CY = 64, 32
EX, EY = CX + 2, CY + 2
NXC, NYC = 1024, 256
LANES = 128
POINTS = 4096
ROWS = POINTS // LANES
CAP = 96
OWNERS = 128
COMP = 2 * EY
PAIR = 6 * COMP
FRONT = 8
TABLE_ROWS = FRONT + (CX + 1) * PAIR + 16
GROUPS = 4
i32, f32, bf16 = jnp.int32, jnp.float32, jnp.bfloat16
VMEM = pl.BlockSpec(memory_space=pltpu.VMEM)
SMEM = pl.BlockSpec(memory_space=pltpu.SMEM)
NT = (((1,), (1,)), ((), ()))


def params():
    return pltpu.CompilerParams(vmem_limit_bytes=60 * 1024 * 1024)


def iota(shape, dim):
    return lax.broadcasted_iota(i32, shape, dim)


def lane_take(x, idx):
    return jnp.take_along_axis(x, idx, axis=1, mode="promise_in_bounds")


def prep_kernel(first, blocks, offs, pix, tile_slot, start, rel, owner, rank, target, sb, so):
    for k in range(4):
        for r in range(ROWS):
            sb[k, r : r + 1, :] = blocks[k : k + 1, r * LANES : (r + 1) * LANES]
    for c in range(3):
        for r in range(ROWS):
            so[c, r : r + 1, :] = offs[c : c + 1, r * LANES : (r + 1) * LANES]
    fx, fy = first[0], first[1]
    lx = [((sb[k] >> 8) - fx + 1) & (NXC - 1) for k in range(4)]
    ly = [((sb[k] & (NYC - 1)) - fy + 1) & (NYC - 1) for k in range(4)]
    qx = jnp.minimum(jnp.minimum(lx[0], lx[1]), jnp.minimum(lx[2], lx[3]))
    qy = jnp.minimum(jnp.minimum(ly[0], ly[1]), jnp.minimum(ly[2], ly[3]))
    odd = (iota((ROWS, LANES), 0) >> 2) & 1
    start[...] = FRONT + qx * PAIR + qy * 2 - 4 * odd
    rel[0] = 2.0 * (so[0] + (lx[0] - qx).astype(f32))
    rel[1] = 2.0 * (so[1] + (ly[0] - qy).astype(f32))
    rel[2] = 2.0 * so[2]
    for i in range(ROWS // 8):
        p = pix[8 * i : 8 * i + 8, :]
        tile = p >> 8
        low, high = tile & (LANES - 1), tile >> 7
        slot = jnp.zeros((8, LANES), i32)
        for t in range(8):
            row = jnp.broadcast_to(tile_slot[t : t + 1, :], (8, LANES))
            slot = jnp.where(high == t, lane_take(row, low), slot)
        owner[8 * i : 8 * i + 8, :] = slot >> 3
        target[8 * i : 8 * i + 8, :] = (slot & 7) * 256 + (p & 255)
    sub = iota((OWNERS, LANES), 0)
    upper = (iota((LANES, 2 * LANES), 0) <= iota((LANES, 2 * LANES), 1)).astype(f32).astype(bf16)

    def step(r, seen):
        hit = sub == jnp.broadcast_to(owner[pl.ds(r, 1), :], (OWNERS, LANES))
        counts = jnp.dot(jnp.where(hit, 1.0, 0.0).astype(bf16), upper, preferred_element_type=f32)
        rank[pl.ds(r, 1), :] = (
            jnp.sum(jnp.where(hit, counts[:, :LANES] + seen, 0.0), axis=0, keepdims=True) - 1.0
        ).astype(i32)
        return seen + counts[:, LANES:]

    lax.fori_loop(0, ROWS, step, jnp.zeros((OWNERS, LANES), f32), unroll=4)


def main_kernel(start, ph, counts, xm, xp, ym, yp, rel, alb, owner, rank, target, send, table, wide, prod, sums, rad):
    lane = iota((CY, LANES), 1)

    def put(c, x, value):
        table[pl.ds(FRONT + (x + 1) * PAIR + c * COMP + 2, CY, stride=2), :] = value
        table[pl.ds(FRONT + x * PAIR + c * COMP + 3, CY, stride=2), :] = value

    def column(x, _):
        at = jnp.full((CY, LANES), x, i32)
        live = lane < lane_take(counts[...], at)
        for c in range(6):
            v = ph[c, x]
            put(c, x, v + v if c < 3 else jnp.where(live, v, 0.0))
        return 0

    lax.fori_loop(0, CX, column, 0, unroll=2)
    for c in range(6):
        scale = 2.0 if c < 3 else 1.0
        table[pl.ds(FRONT + c * COMP + 2, CY, stride=2), :] = xm[c] * scale
        table[pl.ds(FRONT + CX * PAIR + c * COMP + 3, CY, stride=2), :] = xp[c] * scale
        for side, at in ((ym, 0), (yp, 2 * EY - 2)):
            table[pl.ds(FRONT + c * COMP + at, CX + 1, stride=PAIR), :] = side[c, : CX + 1] * scale
            table[pl.ds(FRONT + c * COMP + at + 1, CX + 1, stride=PAIR), :] = side[c, 1:] * scale
    sub = iota((8, LANES), 0)
    upper = sub < 4
    place = ((sub & 1).astype(f32) * 2.0, ((sub >> 1) & 1).astype(f32) * 2.0, None)
    for v in range(4):
        for c in range(3):
            for p in range(4):
                a = jnp.broadcast_to(rel[c, 8 * p + v : 8 * p + v + 1, :], (8, LANES))
                b = jnp.broadcast_to(rel[c, 8 * p + 4 + v : 8 * p + 5 + v, :], (8, LANES))
                both = jnp.where(upper, a, b)
                wide[v, c, p] = both if place[c] is None else both - place[c]

    def block(v, _):
        def groups(g, _):
            for u in range(GROUPS):
                L = g * GROUPS + u
                at = jnp.full((8, LANES), L, i32)
                rows = [start[s * 512 + v * LANES + L] for s in range(8)]
                for p in range(4):
                    ra, rb = rows[2 * p], rows[2 * p + 1]

                    def load(c):
                        return jnp.where(
                            upper, table[pl.ds(ra + c * COMP, 8), :], table[pl.ds(rb + c * COMP, 8), :]
                        )

                    d = [load(c) - lane_take(wide[v, c, p], at) for c in range(3)]
                    dist = d[0] * d[0] + d[1] * d[1] + d[2] * d[2]
                    weight = jnp.maximum(1.0 - dist, 0.0)
                    for c in range(3):
                        prod[u, c, 8 * p : 8 * p + 8, :] = weight * load(3 + c)
                for c in range(3):
                    part = [prod[u, c, pl.ds(i, 8, stride=4), :] for i in range(4)]
                    sums[c, L] = (part[0] + part[1]) + (part[2] + part[3])
            return 0

        lax.fori_loop(0, LANES // GROUPS, groups, 0)
        lanes = iota((8, LANES), 1)

        def reduce(c, first, size):
            if size == 1:
                return sums[c, first]
            half = size // 2
            a, b = reduce(c, first, half), reduce(c, first + half, half)
            mine = (lanes & half) == 0
            return jnp.where(mine, a, b) + pltpu.roll(jnp.where(mine, b, a), half, 1)

        def channel(c, _):
            rad[c, pl.ds(v, 8, stride=4), :] = reduce(c, 0, LANES)
            return 0

        lax.fori_loop(0, 3, channel, 0)
        return 0

    lax.fori_loop(0, 4, block, 0)
    for c in range(3):
        for r in range(ROWS):
            rad[c, r : r + 1, :] = rad[c, r : r + 1, :] * alb[c : c + 1, r * LANES : (r + 1) * LANES]
    wide_sub = iota((OWNERS, 2 * LANES), 0)
    rank_sub = iota((CAP, 2 * LANES), 0)

    def two(ref, r):
        return jnp.concatenate([ref[pl.ds(2 * r, 1), :], ref[pl.ds(2 * r + 1, 1), :]], axis=1)

    def scatter(r, total):
        mine = jnp.where(wide_sub == two(owner, r), 1.0, 0.0).astype(bf16)
        hit = rank_sub == two(rank, r)
        where = two(target, r)
        vals = [two(rad.at[c], r) for c in range(3)]
        high = [x.astype(bf16).astype(f32) for x in vals]
        low = [x - h for x, h in zip(vals, high)]
        high.append((where & ~255).astype(f32))
        low.append((where & 255).astype(f32))
        for part in (high, low):
            rows = jnp.concatenate([jnp.where(hit, x, 0.0) for x in part], axis=0).astype(bf16)
            total = total + lax.dot_general(mine, rows, NT, preferred_element_type=f32)
        return total

    send[...] = lax.fori_loop(0, ROWS // 2, scatter, jnp.zeros((OWNERS, 4 * CAP), f32), unroll=2)


def film_kernel(got, film, flipped, total):
    for j in range(3):
        flipped[LANES * j : LANES * j + LANES, :] = jnp.transpose(got[:, LANES * j : LANES * j + LANES])
    lo_sub = iota((LANES, 2 * LANES), 0)
    hi_sub = iota((16, 2 * LANES), 0)

    def two(row):
        return jnp.concatenate(
            [flipped[pl.ds(row, 1), :], flipped[pl.ds(row + CAP // 2, 1), :]], axis=1
        )

    def step(k, acc):
        where = two(3 * CAP + k).astype(i32)
        low_hit = jnp.where(lo_sub == (where & 127), 1.0, 0.0).astype(bf16)
        hit = hi_sub == (where >> 7)
        high, low = [], []
        for c in range(3):
            x = two(c * CAP + k)
            h = x.astype(bf16).astype(f32)
            high.append(jnp.where(hit, h, 0.0))
            low.append(jnp.where(hit, x - h, 0.0))
        rows = jnp.concatenate(high + low, axis=0).astype(bf16)
        return acc + lax.dot_general(rows, low_hit, NT, preferred_element_type=f32)

    acc = lax.fori_loop(0, CAP // 2, step, jnp.zeros((96, LANES), f32), unroll=4)
    total[...] = acc[:48] + acc[48:]
    for c in range(3):
        film[c, :, :LANES] = total[pl.ds(16 * c, 8, stride=2), :]
        film[c, :, LANES:] = total[pl.ds(16 * c + 1, 8, stride=2), :]


def shift(x, axis, by):
    n = lax.axis_size(axis)
    return lax.ppermute(x, axis, [(i, (i + by) % n) for i in range(n)])


def live_only(x, counts):
    slots = lax.broadcasted_iota(i32, x.shape[1:], x.ndim - 2)
    return jnp.concatenate([x[:3], jnp.where(slots < counts[..., None], x[3:], 0.0)], axis=0)


def per_device(photon_data, block_counts, gather_offsets, gather_blocks, albedo, gather_pixels, tile_slot):
    first = jnp.stack([lax.axis_index("bx") * CX, lax.axis_index("by") * CY]).astype(i32)
    xm = shift(live_only(photon_data[:, -1], block_counts[-1]), "bx", 1)
    xp = shift(live_only(photon_data[:, 0], block_counts[0]), "bx", -1)
    top = live_only(photon_data[:, :, -1], block_counts[:, -1])
    bottom = live_only(photon_data[:, :, 0], block_counts[:, 0])
    ym = shift(jnp.concatenate([xm[:, -1:], top, xp[:, -1:]], axis=1), "by", 1)
    yp = shift(jnp.concatenate([xm[:, :1], bottom, xp[:, :1]], axis=1), "by", -1)
    small_i = jax.ShapeDtypeStruct((ROWS, LANES), i32)
    start, rel, owner, rank, target = pl.pallas_call(
        prep_kernel,
        in_specs=[SMEM, VMEM, VMEM, VMEM, VMEM],
        out_specs=[VMEM] * 5,
        out_shape=[small_i, jax.ShapeDtypeStruct((3, ROWS, LANES), f32), small_i, small_i, small_i],
        scratch_shapes=[pltpu.VMEM((4, ROWS, LANES), i32), pltpu.VMEM((3, ROWS, LANES), f32)],
        compiler_params=params(),
        cost_estimate=pl.CostEstimate(flops=20_000_000, bytes_accessed=300_000, transcendentals=0),
        name="prep",
    )(first, gather_blocks, gather_offsets, gather_pixels.reshape(ROWS, LANES), tile_slot.reshape(8, LANES))
    counts = jnp.pad(block_counts.T, ((0, 0), (0, LANES - CX)))
    send = pl.pallas_call(
        main_kernel,
        in_specs=[SMEM] + [VMEM] * 11,
        out_specs=VMEM,
        out_shape=jax.ShapeDtypeStruct((OWNERS, 4 * CAP), f32),
        scratch_shapes=[
            pltpu.VMEM((TABLE_ROWS, LANES), f32),
            pltpu.VMEM((4, 3, 4, 8, LANES), f32),
            pltpu.VMEM((GROUPS, 3, 32, LANES), f32),
            pltpu.VMEM((3, LANES, 8, LANES), f32),
            pltpu.VMEM((3, ROWS, LANES), f32),
        ],
        compiler_params=params(),
        name="radiance",
    )(start.reshape(POINTS), photon_data, counts, xm, xp, ym, yp, rel, albedo, owner, rank, target)
    got = lax.all_to_all(send, AXES, 0, 0, tiled=True)
    return pl.pallas_call(
        film_kernel,
        in_specs=[VMEM],
        out_specs=VMEM,
        out_shape=jax.ShapeDtypeStruct((3, 8, 256), f32),
        scratch_shapes=[pltpu.VMEM((4 * CAP, LANES), f32), pltpu.VMEM((48, LANES), f32)],
        compiler_params=params(),
        name="film",
    )(got)


def solution(mesh):
    in_specs = (P(None, "bx", "by", None), P("bx", "by"), P(None, AXES), P(None, AXES), P(None, AXES), P(AXES), P())
    return jax.shard_map(per_device, mesh=mesh, in_specs=in_specs, out_specs=P(None, AXES, None), check_vma=False)
```

```python
import jax
import jax.numpy as jnp
from jax import lax
from jax.experimental import pallas as pl
from jax.experimental.pallas import tpu as pltpu
from jax.sharding import PartitionSpec as P

AXES = ("bx", "by")
CX, CY = 64, 32
EX, EY = CX + 2, CY + 2
NXC, NYC = 1024, 256
LANES = 128
POINTS = 4096
ROWS = POINTS // LANES
CAP = 96
OWNERS = 128
TWO = 4 * EY
PAIR = 3 * TWO
TABLE_ROWS = (CX + 1) * PAIR
STEP = 9
GROUPS = 2
i32, f32, bf16 = jnp.int32, jnp.float32, jnp.bfloat16
VMEM = pl.BlockSpec(memory_space=pltpu.VMEM)
SMEM = pl.BlockSpec(memory_space=pltpu.SMEM)
NT = (((1,), (1,)), ((), ()))


def params():
    return pltpu.CompilerParams(vmem_limit_bytes=60 * 1024 * 1024)


def iota(shape, dim):
    return lax.broadcasted_iota(i32, shape, dim)


def lane_take(x, idx):
    return jnp.take_along_axis(x, idx, axis=1, mode="promise_in_bounds")


def prep_kernel(first, blocks, offs, pix, tile_slot, start, rel, owner, rank, target, sb, so):
    for k in range(4):
        for r in range(ROWS):
            sb[k, r : r + 1, :] = blocks[k : k + 1, r * LANES : (r + 1) * LANES]
    for c in range(3):
        for r in range(ROWS):
            so[c, r : r + 1, :] = offs[c : c + 1, r * LANES : (r + 1) * LANES]
    fx, fy = first[0], first[1]
    lx = [((sb[k] >> 8) - fx + 1) & (NXC - 1) for k in range(4)]
    ly = [((sb[k] & (NYC - 1)) - fy + 1) & (NYC - 1) for k in range(4)]
    qx = jnp.minimum(jnp.minimum(lx[0], lx[1]), jnp.minimum(lx[2], lx[3]))
    qy = jnp.minimum(jnp.minimum(ly[0], ly[1]), jnp.minimum(ly[2], ly[3]))
    start[...] = qx * PAIR + qy * 4
    rel[0] = 2.0 * (so[0] + (lx[0] - qx).astype(f32))
    rel[1] = 2.0 * (so[1] + (ly[0] - qy).astype(f32))
    rel[2] = 2.0 * so[2]
    for i in range(ROWS // 8):
        p = pix[8 * i : 8 * i + 8, :]
        tile = p >> 8
        low, high = tile & (LANES - 1), tile >> 7
        slot = jnp.zeros((8, LANES), i32)
        for t in range(8):
            row = jnp.broadcast_to(tile_slot[t : t + 1, :], (8, LANES))
            slot = jnp.where(high == t, lane_take(row, low), slot)
        owner[8 * i : 8 * i + 8, :] = slot >> 3
        target[8 * i : 8 * i + 8, :] = (slot & 7) * 256 + (p & 255)
    sub = iota((OWNERS, LANES), 0)
    upper = (iota((LANES, 2 * LANES), 0) <= iota((LANES, 2 * LANES), 1)).astype(f32).astype(bf16)

    def step(r, seen):
        hit = sub == jnp.broadcast_to(owner[pl.ds(r, 1), :], (OWNERS, LANES))
        counts = jnp.dot(jnp.where(hit, 1.0, 0.0).astype(bf16), upper, preferred_element_type=f32)
        rank[pl.ds(r, 1), :] = (
            jnp.sum(jnp.where(hit, counts[:, :LANES] + seen, 0.0), axis=0, keepdims=True) - 1.0
        ).astype(i32)
        return seen + counts[:, LANES:]

    lax.fori_loop(0, ROWS, step, jnp.zeros((OWNERS, LANES), f32), unroll=4)


def main_kernel(start, ph, counts, xm, xp, ym, yp, rel, alb, owner, rank, target, send, table, stage_a, stage_b, near_a, near_b, sums, rad):
    lane = iota((CY, LANES), 1)

    def row(c, x, y, right):
        return x * PAIR + (c // 2) * TWO + y * 4 + 2 * right + c % 2

    def column(x, _):
        at = jnp.full((CY, LANES), x, i32)
        live = lane < lane_take(counts[...], at)
        for c in range(6):
            v = ph[c, x]
            v = v + v if c < 3 else jnp.where(live, v, 0.0)
            table[pl.ds(row(c, x + 1, 1, 0), CY, stride=4), :] = v
            table[pl.ds(row(c, x, 1, 1), CY, stride=4), :] = v
        return 0

    lax.fori_loop(0, CX, column, 0, unroll=2)
    for c in range(6):
        scale = 2.0 if c < 3 else 1.0
        table[pl.ds(row(c, 0, 1, 0), CY, stride=4), :] = xm[c] * scale
        table[pl.ds(row(c, CX, 1, 1), CY, stride=4), :] = xp[c] * scale
        for side, y in ((ym, 0), (yp, EY - 1)):
            table[pl.ds(row(c, 0, y, 0), CX + 1, stride=PAIR), :] = side[c, : CX + 1] * scale
            table[pl.ds(row(c, 0, y, 1), CX + 1, stride=PAIR), :] = side[c, 1:] * scale
    zero = start[POINTS]

    def fetch(i, stage, near):
        for u in range(GROUPS):
            g = jnp.minimum(i * GROUPS + u, POINTS // 8 - 1)
            at = jnp.full((8, LANES), g & (LANES - 1), i32)
            for c in range(3):
                near[u, c] = lane_take(rel[g >> 7, c], at)
            for s in range(8):
                r = start[g * 8 + s]
                for j in range(3):
                    stage[u, j, pl.ds(zero + STEP * s, 8), :] = table[pl.ds(r + j * TWO, 8), :]

    def weigh(i, stage, near):
        for u in range(GROUPS):
            close = [near[u, c] for c in range(3)]
            far = [x - 2.0 for x in close]
            total = [None] * 3
            for k in range(4):
                yy, xx = k >> 1, k & 1

                def load(c):
                    return stage[u, c // 2, pl.ds(4 * yy + 2 * xx + c % 2, 8, stride=STEP), :]

                o = (far[0] if xx else close[0], far[1] if yy else close[1], close[2])
                d = [load(c) - o[c] for c in range(3)]
                dist = d[0] * d[0] + d[1] * d[1] + d[2] * d[2]
                weight = jnp.maximum(1.0 - dist, 0.0)
                for c in range(3):
                    v = weight * load(3 + c)
                    total[c] = v if k == 0 else total[c] + v
            for c in range(3):
                sums[c, pl.ds(8 * (i * GROUPS + u), 8), :] = total[c]

    def step(i, _):
        weigh(2 * i, stage_a, near_a)
        fetch(2 * i + 1, stage_b, near_b)
        weigh(2 * i + 1, stage_b, near_b)
        fetch(2 * i + 2, stage_a, near_a)
        return 0

    fetch(0, stage_a, near_a)
    trips = POINTS // 16 // GROUPS
    lax.fori_loop(0, trips, step, 0)
    ones = jnp.ones((8, 2 * LANES), f32).astype(bf16)

    def lane_sums(r, _):
        for c in range(3):
            for k in range(2):
                x = sums[c, pl.ds((2 * r + k) * LANES, LANES), :]
                high = x.astype(bf16)
                low = (x - high.astype(f32)).astype(bf16)
                both = jnp.concatenate([high, low], axis=1)
                y = lax.dot_general(ones, both, NT, preferred_element_type=f32)
                rad[c, pl.ds(2 * r + k, 1), :] = y[:1]
        return 0

    lax.fori_loop(0, ROWS // 2, lane_sums, 0)
    for c in range(3):
        for r in range(ROWS):
            rad[c, r : r + 1, :] = rad[c, r : r + 1, :] * alb[c : c + 1, r * LANES : (r + 1) * LANES]
    wide_sub = iota((OWNERS, 2 * LANES), 0)
    rank_sub = iota((CAP, 2 * LANES), 0)

    def two(ref, r):
        return jnp.concatenate([ref[pl.ds(2 * r, 1), :], ref[pl.ds(2 * r + 1, 1), :]], axis=1)

    def scatter(r, total):
        mine = jnp.where(wide_sub == two(owner, r), 1.0, 0.0).astype(bf16)
        hit = rank_sub == two(rank, r)
        where = two(target, r)
        vals = [two(rad.at[c], r) for c in range(3)]
        high = [x.astype(bf16).astype(f32) for x in vals]
        low = [x - h for x, h in zip(vals, high)]
        high.append((where & ~255).astype(f32))
        low.append((where & 255).astype(f32))
        for part in (high, low):
            rows = jnp.concatenate([jnp.where(hit, x, 0.0) for x in part], axis=0).astype(bf16)
            total = total + lax.dot_general(mine, rows, NT, preferred_element_type=f32)
        return total

    send[:, 0, :] = lax.fori_loop(0, ROWS // 2, scatter, jnp.zeros((OWNERS, 4 * CAP), f32), unroll=2)


def film_kernel(got, film, flipped, total):
    for j in range(3):
        flipped[LANES * j : LANES * j + LANES, :] = jnp.transpose(got[:, 0, LANES * j : LANES * j + LANES])
    lo_sub = iota((LANES, 2 * LANES), 0)
    hi_sub = iota((16, 2 * LANES), 0)

    def two(row):
        return jnp.concatenate(
            [flipped[pl.ds(row, 1), :], flipped[pl.ds(row + CAP // 2, 1), :]], axis=1
        )

    def step(k, acc):
        where = two(3 * CAP + k).astype(i32)
        low_hit = jnp.where(lo_sub == (where & 127), 1.0, 0.0).astype(bf16)
        hit = hi_sub == (where >> 7)
        high, low = [], []
        for c in range(3):
            x = two(c * CAP + k)
            h = x.astype(bf16).astype(f32)
            high.append(jnp.where(hit, h, 0.0))
            low.append(jnp.where(hit, x - h, 0.0))
        rows = jnp.concatenate(high + low, axis=0).astype(bf16)
        return acc + lax.dot_general(rows, low_hit, NT, preferred_element_type=f32)

    acc = lax.fori_loop(0, CAP // 2, step, jnp.zeros((96, LANES), f32), unroll=4)
    total[...] = acc[:48] + acc[48:]
    for c in range(3):
        film[c, :, :LANES] = total[pl.ds(16 * c, 8, stride=2), :]
        film[c, :, LANES:] = total[pl.ds(16 * c + 1, 8, stride=2), :]


def shift(x, axis, by):
    n = lax.axis_size(axis)
    return lax.ppermute(x, axis, [(i, (i + by) % n) for i in range(n)])


def live_only(x, counts):
    slots = lax.broadcasted_iota(i32, x.shape[1:], x.ndim - 2)
    return jnp.concatenate([x[:3], jnp.where(slots < counts[..., None], x[3:], 0.0)], axis=0)


def per_device(photon_data, block_counts, gather_offsets, gather_blocks, albedo, gather_pixels, tile_slot):
    first = jnp.stack([lax.axis_index("bx") * CX, lax.axis_index("by") * CY]).astype(i32)
    xm = shift(live_only(photon_data[:, -1], block_counts[-1]), "bx", 1)
    xp = shift(live_only(photon_data[:, 0], block_counts[0]), "bx", -1)
    top = live_only(photon_data[:, :, -1], block_counts[:, -1])
    bottom = live_only(photon_data[:, :, 0], block_counts[:, 0])
    ym = shift(jnp.concatenate([xm[:, -1:], top, xp[:, -1:]], axis=1), "by", 1)
    yp = shift(jnp.concatenate([xm[:, :1], bottom, xp[:, :1]], axis=1), "by", -1)
    small_i = jax.ShapeDtypeStruct((ROWS, LANES), i32)
    start, rel, owner, rank, target = pl.pallas_call(
        prep_kernel,
        in_specs=[SMEM, VMEM, VMEM, VMEM, VMEM],
        out_specs=[VMEM] * 5,
        out_shape=[small_i, jax.ShapeDtypeStruct((3, ROWS, LANES), f32), small_i, small_i, small_i],
        scratch_shapes=[pltpu.VMEM((4, ROWS, LANES), i32), pltpu.VMEM((3, ROWS, LANES), f32)],
        compiler_params=params(),
        cost_estimate=pl.CostEstimate(flops=20_000_000, bytes_accessed=300_000, transcendentals=0),
        name="prep",
    )(first, gather_blocks, gather_offsets, gather_pixels.reshape(ROWS, LANES), tile_slot.reshape(8, LANES))
    rel = rel.reshape(3, 4, LANES, 8).transpose(1, 0, 3, 2)
    counts = jnp.pad(block_counts.T, ((0, 0), (0, LANES - CX)))
    send = pl.pallas_call(
        main_kernel,
        in_specs=[SMEM] + [VMEM] * 11,
        out_specs=VMEM,
        out_shape=jax.ShapeDtypeStruct((OWNERS, 1, 4 * CAP), f32),
        scratch_shapes=[
            pltpu.VMEM((TABLE_ROWS, LANES), f32),
            pltpu.VMEM((GROUPS, 3, 8 * STEP + 8, LANES), f32),
            pltpu.VMEM((GROUPS, 3, 8 * STEP + 8, LANES), f32),
            pltpu.VMEM((GROUPS, 3, 8, LANES), f32),
            pltpu.VMEM((GROUPS, 3, 8, LANES), f32),
            pltpu.VMEM((3, POINTS, LANES), f32),
            pltpu.VMEM((3, ROWS, LANES), f32),
        ],
        compiler_params=params(),
        name="radiance",
    )(jnp.pad(start.reshape(POINTS), (0, LANES)), photon_data, counts, xm, xp, ym, yp, rel, albedo, owner, rank, target)
    got = lax.all_to_all(send, AXES, 0, 0, tiled=True)
    return pl.pallas_call(
        film_kernel,
        in_specs=[VMEM],
        out_specs=VMEM,
        out_shape=jax.ShapeDtypeStruct((3, 8, 256), f32),
        scratch_shapes=[pltpu.VMEM((4 * CAP, LANES), f32), pltpu.VMEM((48, LANES), f32)],
        compiler_params=params(),
        name="film",
    )(got)


def solution(mesh):
    in_specs = (P(None, "bx", "by", None), P("bx", "by"), P(None, AXES), P(None, AXES), P(None, AXES), P(AXES), P())
    return jax.shard_map(per_device, mesh=mesh, in_specs=in_specs, out_specs=P(None, AXES, None), check_vma=False)
```

```python
import jax
import jax.numpy as jnp
from jax import lax
from jax.experimental import pallas as pl
from jax.experimental.pallas import tpu as pltpu
from jax.sharding import PartitionSpec as P

AXES = ("bx", "by")
CX, CY = 64, 32
EX, EY = CX + 2, CY + 2
NXC, NYC = 1024, 256
LANES = 128
POINTS = 4096
ROWS = POINTS // LANES
CAP = 96
OWNERS = 128
TWO = 4 * EY
PAIR = 3 * TWO
TABLE_ROWS = (CX + 1) * PAIR
APART = 513
EDGE_X, EDGE_Y = 4 * EY, 8 * (CX + 1)
EDGE = 2 * EDGE_X + 2 * EDGE_Y
LIST = POINTS + 128
CHUNKS = 8
STEP = 9
GROUPS = 2
i32, f32, bf16 = jnp.int32, jnp.float32, jnp.bfloat16
VMEM = pl.BlockSpec(memory_space=pltpu.VMEM)
SMEM = pl.BlockSpec(memory_space=pltpu.SMEM)
NT = (((1,), (1,)), ((), ()))


HBM = pl.BlockSpec(memory_space=pltpu.HBM)


def params(mib):
    return pltpu.CompilerParams(vmem_limit_bytes=mib * 1024 * 1024)


def iota(shape, dim):
    return lax.broadcasted_iota(i32, shape, dim)


def lane_take(x, idx):
    return jnp.take_along_axis(x, idx, axis=1, mode="promise_in_bounds")


def weigh_eight(stage, close):
    far = [x - 2.0 for x in close]
    total = [None] * 3
    for k in range(4):
        yy, xx = k >> 1, k & 1

        def load(c):
            return stage[c // 2, pl.ds(4 * yy + 2 * xx + c % 2, 8, stride=STEP), :]

        o = (far[0] if xx else close[0], far[1] if yy else close[1], close[2])
        d = [load(c) - o[c] for c in range(3)]
        dist = d[0] * d[0] + d[1] * d[1] + d[2] * d[2]
        weight = jnp.maximum(1.0 - dist, 0.0)
        for c in range(3):
            v = weight * load(3 + c)
            total[c] = v if k == 0 else total[c] + v
    return total


def inner_kernel(ph, counts, blocks, offs, pix, tile_slot, sums, rel, owner, rank, target, points, places,
                 photons, table, sb, so, square, flat, stage_a, stage_b, near_a, near_b, start, psem, ssem):
    part = CX // CHUNKS
    reads = [
        pltpu.make_async_copy(ph.at[:, pl.ds(k * part, part)], photons.at[:, pl.ds(k * part, part)], psem.at[k])
        for k in range(CHUNKS)
    ]
    for read in reads:
        read.start()
    for k in range(4):
        for r in range(ROWS):
            sb[k, r : r + 1, :] = blocks[k : k + 1, r * LANES : (r + 1) * LANES]
    for c in range(3):
        for r in range(ROWS):
            so[c, r : r + 1, :] = offs[c : c + 1, r * LANES : (r + 1) * LANES]
    fx, fy = lax.axis_index("bx") * CX, lax.axis_index("by") * CY
    lx = [((sb[k] >> 8) - fx + 1) & (NXC - 1) for k in range(4)]
    ly = [((sb[k] & (NYC - 1)) - fy + 1) & (NYC - 1) for k in range(4)]
    qx = jnp.minimum(jnp.minimum(lx[0], lx[1]), jnp.minimum(lx[2], lx[3]))
    qy = jnp.minimum(jnp.minimum(ly[0], ly[1]), jnp.minimum(ly[2], ly[3]))
    at = qx * PAIR + qy * 4
    at = jnp.where(qy == CY, -1 - (2 * EDGE_X + EDGE_Y + 8 * qx), at)
    at = jnp.where(qy == 0, -1 - (2 * EDGE_X + 8 * qx), at)
    at = jnp.where(qx == CX, -1 - (EDGE_X + 4 * qy), at)
    at = jnp.where(qx == 0, -1 - 4 * qy, at)
    flat[...] = at
    to_scalar = pltpu.make_async_copy(flat, start, ssem)
    to_scalar.start()
    rel[0] = 2.0 * (so[0] + (lx[0] - qx).astype(f32))
    rel[1] = 2.0 * (so[1] + (ly[0] - qy).astype(f32))
    rel[2] = 2.0 * so[2]
    for i in range(ROWS // 8):
        p = pix[8 * i : 8 * i + 8, :]
        tile = p >> 8
        low, high = tile & (LANES - 1), tile >> 7
        slot = jnp.zeros((8, LANES), i32)
        for t in range(8):
            row = jnp.broadcast_to(tile_slot[t : t + 1, :], (8, LANES))
            slot = jnp.where(high == t, lane_take(row, low), slot)
        owner[8 * i : 8 * i + 8, :] = slot >> 3
        target[8 * i : 8 * i + 8, :] = (slot & 7) * 256 + (p & 255)
    sub = iota((OWNERS, LANES), 0)
    upper = (iota((LANES, 2 * LANES), 0) <= iota((LANES, 2 * LANES), 1)).astype(f32).astype(bf16)

    def ranks(r, seen):
        hit = sub == jnp.broadcast_to(owner[pl.ds(r, 1), :], (OWNERS, LANES))
        tally = jnp.dot(jnp.where(hit, 1.0, 0.0).astype(bf16), upper, preferred_element_type=f32)
        rank[pl.ds(r, 1), :] = (
            jnp.sum(jnp.where(hit, tally[:, :LANES] + seen, 0.0), axis=0, keepdims=True) - 1.0
        ).astype(i32)
        return seen + tally[:, LANES:]

    lax.fori_loop(0, ROWS, ranks, jnp.zeros((OWNERS, LANES), f32), unroll=4)
    square[:CX, :CY] = counts[...].astype(f32)
    filled = jnp.transpose(square[...])[:CY, :].astype(i32)
    lane = iota((CY, LANES), 1)

    def row(c, x, y, right):
        return x * PAIR + (c // 2) * TWO + y * 4 + 2 * right + c % 2

    def column(x, _):
        live = lane < lane_take(filled, jnp.full((CY, LANES), x, i32))
        for c in range(6):
            v = photons[c, x]
            v = v + v if c < 3 else jnp.where(live, v, 0.0)
            table[pl.ds(row(c, x + 1, 1, 0), CY, stride=4), :] = v
            table[pl.ds(row(c, x, 1, 1), CY, stride=4), :] = v
        return 0

    for k in range(CHUNKS):
        reads[k].wait()
        lax.fori_loop(k * part, (k + 1) * part, column, 0, unroll=2)
    to_scalar.wait()
    zero = lax.axis_index("bx") * 0

    def fetch(i, count, stage, near):
        for u in range(GROUPS):
            g = jnp.minimum(i * GROUPS + u, POINTS // 8 - 1)
            v, lane = g >> 7, g & (LANES - 1)
            take = jnp.full((8, LANES), lane, i32)
            for c in range(3):
                near[u, c] = lane_take(rel[c, pl.ds(v, 8, stride=4), :], take)
            for s in range(8):
                at = start[4 * s + v, lane]
                points[count] = g + 512 * s
                places[count] = -1 - at
                count = count + lax.shift_right_logical(at, 31)
                r = jnp.maximum(at, 0)
                for j in range(3):
                    stage[u, j, pl.ds(zero + STEP * s, 8), :] = table[pl.ds(r + j * TWO, 8), :]
        return count

    def weigh(i, stage, near):
        for u in range(GROUPS):
            total = weigh_eight(stage.at[u], [near[u, c] for c in range(3)])
            for c in range(3):
                sums[c, pl.ds(i * GROUPS + u, 8, stride=APART), :] = total[c]

    def step(i, count):
        weigh(2 * i, stage_a, near_a)
        count = fetch(2 * i + 1, count, stage_b, near_b)
        weigh(2 * i + 1, stage_b, near_b)
        return fetch(2 * i + 2, count, stage_a, near_a)

    count = fetch(0, 0, stage_a, near_a)
    points[LIST - 1] = lax.fori_loop(0, POINTS // 16 // GROUPS, step, count)


def outer_kernel(points, places, sums, rel, alb, owner, rank, target, xm, xp, c0, c63, ym, yp, bottom, top,
                 send, edge, stage, rad):
    for c in range(6):
        scale = 2.0 if c < 3 else 1.0
        plane = (c // 2) * EDGE + c % 2
        for base, cols in ((0, ((xm, 0), (c0, 1))), (EDGE_X, ((c63, CX), (xp, CX + 1)))):
            for right, (col, x) in enumerate(cols):
                at = plane + base + 2 * right
                edge[pl.ds(at + 4, CY, stride=4), :] = col[c] * scale
                edge[at : at + 1, :] = ym[c, x : x + 1] * scale
                edge[at + 4 * EY - 4 : at + 4 * EY - 3, :] = yp[c, x : x + 1] * scale
        for base, lines in ((2 * EDGE_X, (ym, bottom)), (2 * EDGE_X + EDGE_Y, (top, yp))):
            for yy, line in enumerate(lines):
                for right in range(2):
                    at = plane + base + 4 * yy + 2 * right
                    edge[pl.ds(at, CX + 1, stride=8), :] = line[c, right : right + CX + 1] * scale
    sub = iota((8, LANES), 0)
    zero = lax.axis_index("bx") * 0
    count = points[LIST - 1]

    def eight(i, _):
        close = [jnp.zeros((8, LANES), f32)] * 3
        where = []
        for s in range(8):
            k = jnp.minimum(8 * i + s, count - 1)
            p, r = points[k], places[k]
            where.append((p >> 9) * APART + (p & 511))
            take = jnp.full((8, LANES), p & (LANES - 1), i32)
            for c in range(3):
                line = jnp.broadcast_to(rel[c, pl.ds(p >> 7, 1), :], (8, LANES))
                close[c] = jnp.where(sub == s, lane_take(line, take), close[c])
            for j in range(3):
                stage[j, pl.ds(zero + STEP * s, 8), :] = edge[pl.ds(r + j * EDGE, 8), :]
        total = weigh_eight(stage, close)
        for c in range(3):
            for s in range(8):
                sums[c, pl.ds(where[s], 1), :] = total[c][s : s + 1]
        return 0

    lax.fori_loop(0, (count + 7) >> 3, eight, 0)
    ones = jnp.ones((8, 2 * LANES), f32).astype(bf16)

    def lane_sums(r, _):
        for c in range(3):
            for k in range(2):
                line = 2 * r + k
                x = sums[c, pl.ds((line >> 2) * APART + (line & 3) * LANES, LANES), :]
                high = x.astype(bf16)
                low = (x - high.astype(f32)).astype(bf16)
                both = jnp.concatenate([high, low], axis=1)
                y = lax.dot_general(ones, both, NT, preferred_element_type=f32)
                rad[c, pl.ds(line, 1), :] = y[:1]
        return 0

    lax.fori_loop(0, ROWS // 2, lane_sums, 0)
    for c in range(3):
        for r in range(ROWS):
            rad[c, r : r + 1, :] = rad[c, r : r + 1, :] * alb[c : c + 1, r * LANES : (r + 1) * LANES]
    wide_sub = iota((OWNERS, 2 * LANES), 0)
    rank_sub = iota((CAP, 2 * LANES), 0)

    def two(ref, r):
        return jnp.concatenate([ref[pl.ds(2 * r, 1), :], ref[pl.ds(2 * r + 1, 1), :]], axis=1)

    def scatter(r, total):
        mine = jnp.where(wide_sub == two(owner, r), 1.0, 0.0).astype(bf16)
        hit = rank_sub == two(rank, r)
        where = two(target, r)
        vals = [two(rad.at[c], r) for c in range(3)]
        high = [x.astype(bf16).astype(f32) for x in vals]
        low = [x - h for x, h in zip(vals, high)]
        high.append((where & ~255).astype(f32))
        low.append((where & 255).astype(f32))
        for part in (high, low):
            rows = jnp.concatenate([jnp.where(hit, x, 0.0) for x in part], axis=0).astype(bf16)
            total = total + lax.dot_general(mine, rows, NT, preferred_element_type=f32)
        return total

    send[:, 0, :] = lax.fori_loop(0, ROWS // 2, scatter, jnp.zeros((OWNERS, 4 * CAP), f32), unroll=2)


def film_kernel(got, film, flipped, total):
    for j in range(3):
        flipped[LANES * j : LANES * j + LANES, :] = jnp.transpose(got[:, 0, LANES * j : LANES * j + LANES])
    lo_sub = iota((LANES, 2 * LANES), 0)
    hi_sub = iota((16, 2 * LANES), 0)

    def two(row):
        return jnp.concatenate(
            [flipped[pl.ds(row, 1), :], flipped[pl.ds(row + CAP // 2, 1), :]], axis=1
        )

    def step(k, acc):
        where = two(3 * CAP + k).astype(i32)
        low_hit = jnp.where(lo_sub == (where & 127), 1.0, 0.0).astype(bf16)
        hit = hi_sub == (where >> 7)
        high, low = [], []
        for c in range(3):
            x = two(c * CAP + k)
            h = x.astype(bf16).astype(f32)
            high.append(jnp.where(hit, h, 0.0))
            low.append(jnp.where(hit, x - h, 0.0))
        rows = jnp.concatenate(high + low, axis=0).astype(bf16)
        return acc + lax.dot_general(rows, low_hit, NT, preferred_element_type=f32)

    acc = lax.fori_loop(0, CAP // 2, step, jnp.zeros((96, LANES), f32), unroll=4)
    total[...] = acc[:48] + acc[48:]
    for c in range(3):
        film[c, :, :LANES] = total[pl.ds(16 * c, 8, stride=2), :]
        film[c, :, LANES:] = total[pl.ds(16 * c + 1, 8, stride=2), :]


def shift(x, axis, by):
    n = lax.axis_size(axis)
    return lax.ppermute(x, axis, [(i, (i + by) % n) for i in range(n)])


def live_only(x, counts):
    slots = lax.broadcasted_iota(i32, x.shape[1:], x.ndim - 2)
    return jnp.concatenate([x[:3], jnp.where(slots < counts[..., None], x[3:], 0.0)], axis=0)


def per_device(photon_data, block_counts, gather_offsets, gather_blocks, albedo, gather_pixels, tile_slot):
    small_i = jax.ShapeDtypeStruct((ROWS, LANES), i32)
    listed = jax.ShapeDtypeStruct((LIST,), i32)
    c63 = live_only(photon_data[:, -1], block_counts[-1])
    c0 = live_only(photon_data[:, 0], block_counts[0])
    xm, xp = shift(c63, "bx", 1), shift(c0, "bx", -1)
    top = live_only(photon_data[:, :, -1], block_counts[:, -1])
    bottom = live_only(photon_data[:, :, 0], block_counts[:, 0])
    top = jnp.concatenate([xm[:, -1:], top, xp[:, -1:]], axis=1)
    bottom = jnp.concatenate([xm[:, :1], bottom, xp[:, :1]], axis=1)
    ym, yp = shift(top, "by", 1), shift(bottom, "by", -1)
    sums, rel, owner, rank, target, points, places = pl.pallas_call(
        inner_kernel,
        in_specs=[HBM] + [VMEM] * 5,
        out_specs=[VMEM] * 5 + [SMEM] * 2,
        out_shape=[
            jax.ShapeDtypeStruct((3, 8 * APART, LANES), f32),
            jax.ShapeDtypeStruct((3, ROWS, LANES), f32),
            small_i, small_i, small_i, listed, listed,
        ],
        scratch_shapes=[
            pltpu.VMEM((6, CX, CY, LANES), f32),
            pltpu.VMEM((TABLE_ROWS, LANES), f32),
            pltpu.VMEM((4, ROWS, LANES), i32),
            pltpu.VMEM((3, ROWS, LANES), f32),
            pltpu.VMEM((LANES, LANES), f32),
            pltpu.VMEM((ROWS, LANES), i32),
            pltpu.VMEM((GROUPS, 3, 8 * STEP + 8, LANES), f32),
            pltpu.VMEM((GROUPS, 3, 8 * STEP + 8, LANES), f32),
            pltpu.VMEM((GROUPS, 3, 8, LANES), f32),
            pltpu.VMEM((GROUPS, 3, 8, LANES), f32),
            pltpu.SMEM((ROWS, LANES), i32),
            pltpu.SemaphoreType.DMA((CHUNKS,)),
            pltpu.SemaphoreType.DMA,
        ],
        compiler_params=params(34),
        cost_estimate=pl.CostEstimate(flops=60_000_000, bytes_accessed=7_000_000, transcendentals=0),
        name="inner",
    )(photon_data, block_counts, gather_blocks, gather_offsets,
      gather_pixels.reshape(ROWS, LANES), tile_slot.reshape(8, LANES))
    send = pl.pallas_call(
        outer_kernel,
        in_specs=[SMEM] * 2 + [VMEM] * 14,
        out_specs=VMEM,
        out_shape=jax.ShapeDtypeStruct((OWNERS, 1, 4 * CAP), f32),
        scratch_shapes=[
            pltpu.VMEM((3 * EDGE + 8, LANES), f32),
            pltpu.VMEM((3, 8 * STEP + 8, LANES), f32),
            pltpu.VMEM((3, ROWS, LANES), f32),
        ],
        compiler_params=params(16),
        name="outer",
    )(points, places, sums, rel, albedo, owner, rank, target, xm, xp, c0, c63, ym, yp, bottom, top)
    got = lax.all_to_all(send, AXES, 0, 0, tiled=True)
    return pl.pallas_call(
        film_kernel,
        in_specs=[VMEM],
        out_specs=VMEM,
        out_shape=jax.ShapeDtypeStruct((3, 8, 256), f32),
        scratch_shapes=[pltpu.VMEM((4 * CAP, LANES), f32), pltpu.VMEM((48, LANES), f32)],
        compiler_params=params(16),
        name="film",
    )(got)


def solution(mesh):
    in_specs = (P(None, "bx", "by", None), P("bx", "by"), P(None, AXES), P(None, AXES), P(None, AXES), P(AXES), P())
    return jax.shard_map(per_device, mesh=mesh, in_specs=in_specs, out_specs=P(None, AXES, None), check_vma=False)
```

```python
import jax
import jax.numpy as jnp
from jax import lax
from jax.experimental import pallas as pl
from jax.experimental.pallas import tpu as pltpu
from jax.sharding import PartitionSpec as P

AXES = ("bx", "by")
CX, CY = 64, 32
EX, EY = CX + 2, CY + 2
NXC, NYC = 1024, 256
LANES = 128
POINTS = 4096
ROWS = POINTS // LANES
CAP = 96
OWNERS = 128
TWO = 4 * EY
PAIR = 3 * TWO
TABLE_ROWS = (CX + 1) * PAIR
APART = 513
EDGE_X, EDGE_Y = 4 * EY, 8 * (CX + 1)
EDGE = 2 * EDGE_X + 2 * EDGE_Y
LIST = ROWS + 8
STEP = 9
GROUPS = 4
i32, f32, bf16 = jnp.int32, jnp.float32, jnp.bfloat16
VMEM = pl.BlockSpec(memory_space=pltpu.VMEM)
SMEM = pl.BlockSpec(memory_space=pltpu.SMEM)
NT = (((1,), (1,)), ((), ()))


HBM = pl.BlockSpec(memory_space=pltpu.HBM)


def params(mib):
    return pltpu.CompilerParams(vmem_limit_bytes=int(mib * 1024 * 1024))


def iota(shape, dim):
    return lax.broadcasted_iota(i32, shape, dim)


def lane_take(x, idx):
    return jnp.take_along_axis(x, idx, axis=1, mode="promise_in_bounds")


def weigh_eight(stage, close):
    far = [x - 2.0 for x in close]
    total = [None] * 3
    for k in range(4):
        yy, xx = k >> 1, k & 1

        def load(c):
            return stage[c // 2, pl.ds(4 * yy + 2 * xx + c % 2, 8, stride=STEP), :]

        o = (far[0] if xx else close[0], far[1] if yy else close[1], close[2])
        d = [load(c) - o[c] for c in range(3)]
        dist = d[0] * d[0] + d[1] * d[1] + d[2] * d[2]
        weight = jnp.maximum(1.0 - dist, 0.0)
        for c in range(3):
            v = weight * load(3 + c)
            total[c] = v if k == 0 else total[c] + v
    return total


def prep_kernel(ph, counts, blocks, offs, pix, tile_slot,
                c63, c0, top, bottom, flat, rel, owner, rank, target, points, places, square, sb, so, where):
    square[:CX, :CY] = counts[...].astype(f32)
    by_x = square[:CX, :].astype(i32)
    by_y = jnp.transpose(square[...])[:CY, :].astype(i32)
    for out, x in ((c63, CX - 1), (c0, 0)):
        live = iota((CY, LANES), 1) < lane_take(by_y, jnp.full((CY, LANES), x, i32))
        for c in range(6):
            v = ph[c, x]
            out[c] = v if c < 3 else jnp.where(live, v, 0.0)
    for out, y in ((top, CY - 1), (bottom, 0)):
        live = iota((CX, LANES), 1) < lane_take(by_x, jnp.full((CX, LANES), y, i32))
        for c in range(6):
            v = ph[c, :, y, :]
            out[c] = v if c < 3 else jnp.where(live, v, 0.0)
    for k in range(4):
        for r in range(ROWS):
            sb[k, r : r + 1, :] = blocks[k : k + 1, r * LANES : (r + 1) * LANES]
    for c in range(3):
        for r in range(ROWS):
            so[c, r : r + 1, :] = offs[c : c + 1, r * LANES : (r + 1) * LANES]
    fx, fy = lax.axis_index("bx") * CX, lax.axis_index("by") * CY
    lx = [((sb[k] >> 8) - fx + 1) & (NXC - 1) for k in range(4)]
    ly = [((sb[k] & (NYC - 1)) - fy + 1) & (NYC - 1) for k in range(4)]
    qx = jnp.minimum(jnp.minimum(lx[0], lx[1]), jnp.minimum(lx[2], lx[3]))
    qy = jnp.minimum(jnp.minimum(ly[0], ly[1]), jnp.minimum(ly[2], ly[3]))
    at = qx * PAIR + qy * 4
    at = jnp.where(qy == CY, -1 - (2 * EDGE_X + EDGE_Y + 8 * qx), at)
    at = jnp.where(qy == 0, -1 - (2 * EDGE_X + 8 * qx), at)
    at = jnp.where(qx == CX, -1 - (EDGE_X + 4 * qy), at)
    at = jnp.where(qx == 0, -1 - 4 * qy, at)
    flat[...] = jnp.maximum(at, 0)
    rel[0] = 2.0 * (so[0] + (lx[0] - qx).astype(f32))
    rel[1] = 2.0 * (so[1] + (ly[0] - qy).astype(f32))
    rel[2] = 2.0 * so[2]
    for i in range(ROWS // 8):
        p = pix[8 * i : 8 * i + 8, :]
        tile = p >> 8
        low, high = tile & (LANES - 1), tile >> 7
        slot = jnp.zeros((8, LANES), i32)
        for t in range(8):
            row = jnp.broadcast_to(tile_slot[t : t + 1, :], (8, LANES))
            slot = jnp.where(high == t, lane_take(row, low), slot)
        owner[8 * i : 8 * i + 8, :] = slot >> 3
        target[8 * i : 8 * i + 8, :] = (slot & 7) * 256 + (p & 255)
    sub = iota((OWNERS, LANES), 0)
    upper = (iota((LANES, 2 * LANES), 0) <= iota((LANES, 2 * LANES), 1)).astype(f32).astype(bf16)

    def ranks(r, seen):
        hit = sub == jnp.broadcast_to(owner[pl.ds(r, 1), :], (OWNERS, LANES))
        tally = jnp.dot(jnp.where(hit, 1.0, 0.0).astype(bf16), upper, preferred_element_type=f32)
        rank[pl.ds(r, 1), :] = (
            jnp.sum(jnp.where(hit, tally[:, :LANES] + seen, 0.0), axis=0, keepdims=True) - 1.0
        ).astype(i32)
        return seen + tally[:, LANES:]

    lax.fori_loop(0, ROWS, ranks, jnp.zeros((OWNERS, LANES), f32), unroll=16)
    outside = at < 0
    tally = jnp.dot(jnp.where(outside, 1.0, 0.0).astype(bf16), upper, preferred_element_type=f32)
    before = iota((ROWS, ROWS), 1) < iota((ROWS, ROWS), 0)
    ahead = jnp.dot(
        jnp.where(before, 1.0, 0.0).astype(bf16), tally[:, LANES:].astype(bf16), preferred_element_type=f32
    )
    count = (ahead + tally[:, LANES:])[ROWS - 1 :].astype(i32)
    where[0] = jnp.where(outside, (ahead + tally[:, :LANES] - 1.0).astype(i32), -1)
    where[1] = iota((ROWS, LANES), 0) * LANES + iota((ROWS, LANES), 1)
    where[2] = -1 - at
    low_sub = iota((LANES, 2 * LANES), 0)
    high_sub = iota((ROWS, 2 * LANES), 0)

    def collect(r, total):
        spot, point, place = [
            jnp.concatenate([where[k, pl.ds(2 * r, 1), :], where[k, pl.ds(2 * r + 1, 1), :]], axis=1)
            for k in range(3)
        ]
        low_hit = jnp.where(low_sub == (spot & (LANES - 1)), 1.0, 0.0).astype(bf16)
        hit = high_sub == (spot >> 7)
        parts = [(point >> 8), (point & 255), (place >> 8), (place & 255)]
        rows = jnp.concatenate([jnp.where(hit, x.astype(f32), 0.0) for x in parts], axis=0).astype(bf16)
        return total + lax.dot_general(rows, low_hit, NT, preferred_element_type=f32)

    found = lax.fori_loop(0, ROWS // 2, collect, jnp.zeros((4 * ROWS, LANES), f32), unroll=8).astype(i32)
    points[:ROWS] = found[:ROWS] * 256 + found[ROWS : 2 * ROWS]
    places[:ROWS] = found[2 * ROWS : 3 * ROWS] * 256 + found[3 * ROWS :]
    points[ROWS:] = jnp.broadcast_to(count, (8, LANES))
    places[ROWS:] = jnp.broadcast_to(count, (8, LANES))

def inner_kernel(ph, counts, flat, rel, sums, near, table, square, stage_a, stage_b, ssem, *start):
    to_scalar = [pltpu.make_async_copy(flat.at[pl.ds(4 * s, 4)], start[s], ssem.at[s]) for s in range(8)]
    for copy in to_scalar:
        copy.start()
    square[:CX, :CY] = counts[...].astype(f32)
    filled = jnp.transpose(square[...])[:CY, :].astype(i32)
    lane = iota((CY, LANES), 1)

    def row(c, x, y, right):
        return x * PAIR + (c // 2) * TWO + y * 4 + 2 * right + c % 2

    def column(x, _):
        live = lane < lane_take(filled, jnp.full((CY, LANES), x, i32))
        for c in range(6):
            v = ph[c, x]
            v = v + v if c < 3 else jnp.where(live, v, 0.0)
            table[pl.ds(row(c, x + 1, 1, 0), CY, stride=4), :] = v
            table[pl.ds(row(c, x, 1, 1), CY, stride=4), :] = v
        return 0

    lax.fori_loop(0, CX, column, 0, unroll=8)
    for copy in to_scalar:
        copy.wait()
    zero = lax.axis_index("bx") * 0

    parts = [[rel[c, pl.ds(v, 8, stride=4), :] for c in range(3)] for v in range(4)]

    def spread(lane, _):
        take = jnp.full((8, LANES), lane, i32)
        for v in range(4):
            for c in range(3):
                near[c, v * LANES + lane] = lane_take(parts[v][c], take)
        return 0

    lax.fori_loop(0, LANES, spread, 0, unroll=8)

    def fetch(i, stage):
        for u in range(GROUPS):
            g = jnp.minimum(i * GROUPS + u, POINTS // 8 - 1)
            v, lane = g >> 7, g & (LANES - 1)
            for s in range(8):
                r = start[s][v, lane]
                for j in range(3):
                    stage[u, j, pl.ds(zero + STEP * s, 8), :] = table[pl.ds(r + j * TWO, 8), :]

    def weigh(i, stage):
        for u in range(GROUPS):
            total = weigh_eight(stage.at[u], [near[c, i * GROUPS + u] for c in range(3)])
            for c in range(3):
                sums[c, pl.ds(i * GROUPS + u, 8, stride=APART), :] = total[c]

    def step(i, _):
        weigh(2 * i, stage_a)
        fetch(2 * i + 1, stage_b)
        weigh(2 * i + 1, stage_b)
        fetch(2 * i + 2, stage_a)
        return 0

    fetch(0, stage_a)
    lax.fori_loop(0, POINTS // 16 // GROUPS, step, 0)


def outer_kernel(points, places, sums, near, alb, owner, rank, target, xm, xp, c0, c63, ym, yp, bottom, top,
                 send, edge, stage, close, rad):
    for c in range(6):
        scale = 2.0 if c < 3 else 1.0
        plane = (c // 2) * EDGE + c % 2
        for base, cols in ((0, ((xm, 0), (c0, 1))), (EDGE_X, ((c63, CX), (xp, CX + 1)))):
            for right, (col, x) in enumerate(cols):
                at = plane + base + 2 * right
                edge[pl.ds(at + 4, CY, stride=4), :] = col[c] * scale
                edge[at : at + 1, :] = ym[c, x : x + 1] * scale
                edge[at + 4 * EY - 4 : at + 4 * EY - 3, :] = yp[c, x : x + 1] * scale
        for base, lines in ((2 * EDGE_X, (ym, bottom)), (2 * EDGE_X + EDGE_Y, (top, yp))):
            for yy, line in enumerate(lines):
                for right in range(2):
                    at = plane + base + 4 * yy + 2 * right
                    edge[pl.ds(at, CX + 1, stride=8), :] = line[c, right : right + CX + 1] * scale
    sub = iota((8, LANES), 0)
    zero = lax.axis_index("bx") * 0
    count = points[ROWS, 0]

    def eight(i, _):
        where = []
        for s in range(8):
            k = jnp.minimum(8 * i + s, count - 1)
            p, r = points[k >> 7, k & (LANES - 1)], places[k >> 7, k & (LANES - 1)]
            where.append((p >> 9) * APART + (p & 511))
            for c in range(3):
                close[c, s : s + 1, :] = near[c, p & 511, pl.ds(p >> 9, 1), :]
            for j in range(3):
                stage[j, pl.ds(zero + STEP * s, 8), :] = edge[pl.ds(r + j * EDGE, 8), :]
        total = weigh_eight(stage, [close[c] for c in range(3)])
        for c in range(3):
            for s in range(8):
                sums[c, pl.ds(where[s], 1), :] = total[c][s : s + 1]
        return 0

    lax.fori_loop(0, (count + 7) >> 3, eight, 0)
    ones = jnp.ones((8, 2 * LANES), f32).astype(bf16)

    def lane_sums(r, _):
        for c in range(3):
            for k in range(2):
                line = 2 * r + k
                x = sums[c, pl.ds((line >> 2) * APART + (line & 3) * LANES, LANES), :]
                high = x.astype(bf16)
                low = (x - high.astype(f32)).astype(bf16)
                both = jnp.concatenate([high, low], axis=1)
                y = lax.dot_general(ones, both, NT, preferred_element_type=f32)
                rad[c, pl.ds(line, 1), :] = y[:1]
        return 0

    lax.fori_loop(0, ROWS // 2, lane_sums, 0, unroll=8)
    for c in range(3):
        for r in range(ROWS):
            rad[c, r : r + 1, :] = rad[c, r : r + 1, :] * alb[c : c + 1, r * LANES : (r + 1) * LANES]
    wide_sub = iota((OWNERS, 2 * LANES), 0)
    rank_sub = iota((CAP, 2 * LANES), 0)

    def two(ref, r):
        return jnp.concatenate([ref[pl.ds(2 * r, 1), :], ref[pl.ds(2 * r + 1, 1), :]], axis=1)

    def scatter(r, total):
        mine = jnp.where(wide_sub == two(owner, r), 1.0, 0.0).astype(bf16)
        hit = rank_sub == two(rank, r)
        where = two(target, r)
        vals = [two(rad.at[c], r) for c in range(3)]
        high = [x.astype(bf16).astype(f32) for x in vals]
        low = [x - h for x, h in zip(vals, high)]
        high.append((where & ~255).astype(f32))
        low.append((where & 255).astype(f32))
        for part in (high, low):
            rows = jnp.concatenate([jnp.where(hit, x, 0.0) for x in part], axis=0).astype(bf16)
            total = total + lax.dot_general(mine, rows, NT, preferred_element_type=f32)
        return total

    send[:, 0, :] = lax.fori_loop(0, ROWS // 2, scatter, jnp.zeros((OWNERS, 4 * CAP), f32), unroll=8)


def film_kernel(got, film, flipped, total):
    for j in range(3):
        flipped[LANES * j : LANES * j + LANES, :] = jnp.transpose(got[:, 0, LANES * j : LANES * j + LANES])
    lo_sub = iota((LANES, 2 * LANES), 0)
    hi_sub = iota((16, 2 * LANES), 0)

    def two(row):
        return jnp.concatenate(
            [flipped[pl.ds(row, 1), :], flipped[pl.ds(row + CAP // 2, 1), :]], axis=1
        )

    def step(k, acc):
        where = two(3 * CAP + k).astype(i32)
        low_hit = jnp.where(lo_sub == (where & 127), 1.0, 0.0).astype(bf16)
        hit = hi_sub == (where >> 7)
        high, low = [], []
        for c in range(3):
            x = two(c * CAP + k)
            h = x.astype(bf16).astype(f32)
            high.append(jnp.where(hit, h, 0.0))
            low.append(jnp.where(hit, x - h, 0.0))
        rows = jnp.concatenate(high + low, axis=0).astype(bf16)
        return acc + lax.dot_general(rows, low_hit, NT, preferred_element_type=f32)

    acc = lax.fori_loop(0, CAP // 2, step, jnp.zeros((96, LANES), f32), unroll=16)
    total[...] = acc[:48] + acc[48:]
    for c in range(3):
        film[c, :, :LANES] = total[pl.ds(16 * c, 8, stride=2), :]
        film[c, :, LANES:] = total[pl.ds(16 * c + 1, 8, stride=2), :]


def shift(x, axis, by):
    n = lax.axis_size(axis)
    return lax.ppermute(x, axis, [(i, (i + by) % n) for i in range(n)])


def per_device(photon_data, block_counts, gather_offsets, gather_blocks, albedo, gather_pixels, tile_slot):
    small_i = jax.ShapeDtypeStruct((ROWS, LANES), i32)
    listed = jax.ShapeDtypeStruct((LIST, LANES), i32)
    column, line = jax.ShapeDtypeStruct((6, CY, LANES), f32), jax.ShapeDtypeStruct((6, CX, LANES), f32)
    c63, c0, top, bottom, flat, rel, owner, rank, target, points, places = pl.pallas_call(
        prep_kernel,
        in_specs=[VMEM] * 6,
        out_specs=[VMEM] * 11,
        out_shape=[column, column, line, line]
        + [small_i, jax.ShapeDtypeStruct((3, ROWS, LANES), f32), small_i, small_i, small_i, listed, listed],
        scratch_shapes=[
            pltpu.VMEM((LANES, LANES), f32),
            pltpu.VMEM((4, ROWS, LANES), i32),
            pltpu.VMEM((3, ROWS, LANES), f32),
            pltpu.VMEM((3, ROWS, LANES), i32),
        ],
        compiler_params=params(16),
        cost_estimate=pl.CostEstimate(flops=20_000_000, bytes_accessed=300_000, transcendentals=0),
        name="prep",
    )(photon_data, block_counts, gather_blocks, gather_offsets,
      gather_pixels.reshape(ROWS, LANES), tile_slot.reshape(8, LANES))
    xm, xp = shift(c63, "bx", 1), shift(c0, "bx", -1)
    top = jnp.concatenate([xm[:, -1:], top, xp[:, -1:]], axis=1)
    bottom = jnp.concatenate([xm[:, :1], bottom, xp[:, :1]], axis=1)
    ym, yp = shift(top, "by", 1), shift(bottom, "by", -1)
    sums, near = pl.pallas_call(
        inner_kernel,
        in_specs=[VMEM] * 4,
        out_specs=[VMEM] * 2,
        out_shape=[
            jax.ShapeDtypeStruct((3, 8 * APART, LANES), f32),
            jax.ShapeDtypeStruct((3, POINTS // 8, 8, LANES), f32),
        ],
        scratch_shapes=[
            pltpu.VMEM((TABLE_ROWS, LANES), f32),
            pltpu.VMEM((LANES, LANES), f32),
            pltpu.VMEM((GROUPS, 3, 8 * STEP + 8, LANES), f32),
            pltpu.VMEM((GROUPS, 3, 8 * STEP + 8, LANES), f32),
            pltpu.SemaphoreType.DMA((8,)),
        ]
        + [pltpu.SMEM((4, LANES), i32)] * 8,
        compiler_params=params(34),
        cost_estimate=pl.CostEstimate(flops=60_000_000, bytes_accessed=7_000_000, transcendentals=0),
        name="inner",
    )(photon_data, block_counts, flat, rel)
    send = pl.pallas_call(
        outer_kernel,
        in_specs=[SMEM] * 2 + [VMEM] * 14,
        out_specs=VMEM,
        out_shape=jax.ShapeDtypeStruct((OWNERS, 1, 4 * CAP), f32),
        scratch_shapes=[
            pltpu.VMEM((3 * EDGE + 64, LANES), f32),
            pltpu.VMEM((3, 8 * STEP + 8, LANES), f32),
            pltpu.VMEM((3, 8, LANES), f32),
            pltpu.VMEM((3, ROWS, LANES), f32),
        ],
        compiler_params=params(16),
        name="outer",
    )(points, places, sums, near, albedo, owner, rank, target, xm, xp, c0, c63, ym, yp, bottom, top)
    got = lax.all_to_all(send, AXES, 0, 0, tiled=True)
    return pl.pallas_call(
        film_kernel,
        in_specs=[VMEM],
        out_specs=VMEM,
        out_shape=jax.ShapeDtypeStruct((3, 8, 256), f32),
        scratch_shapes=[pltpu.VMEM((4 * CAP, LANES), f32), pltpu.VMEM((48, LANES), f32)],
        compiler_params=params(16),
        name="film",
    )(got)


def solution(mesh):
    in_specs = (P(None, "bx", "by", None), P("bx", "by"), P(None, AXES), P(None, AXES), P(None, AXES), P(AXES), P())
    return jax.shard_map(per_device, mesh=mesh, in_specs=in_specs, out_specs=P(None, AXES, None), check_vma=False)
```

```python
import jax
import jax.numpy as jnp
from jax import lax
from jax.experimental import pallas as pl
from jax.experimental.pallas import tpu as pltpu
from jax.sharding import PartitionSpec as P

AXES = ("bx", "by")
CX, CY = 64, 32
EX, EY = CX + 2, CY + 2
NXC, NYC = 1024, 256
LANES = 128
POINTS = 4096
ROWS = POINTS // LANES
CAP = 96
OWNERS = 128
TWO = 4 * EY
PAIR = 3 * TWO
TABLE_ROWS = (CX + 1) * PAIR
APART = 513
EDGE_X, EDGE_Y = 4 * EY, 8 * (CX + 1)
EDGE = 2 * EDGE_X + 2 * EDGE_Y
LIST = ROWS + 8
STEP = 9
TOGETHER = 4
GROUPS = 4
i32, f32, bf16 = jnp.int32, jnp.float32, jnp.bfloat16
VMEM = pl.BlockSpec(memory_space=pltpu.VMEM)
SMEM = pl.BlockSpec(memory_space=pltpu.SMEM)
NT = (((1,), (1,)), ((), ()))


HBM = pl.BlockSpec(memory_space=pltpu.HBM)


def params(mib):
    return pltpu.CompilerParams(vmem_limit_bytes=int(mib * 1024 * 1024))


def iota(shape, dim):
    return lax.broadcasted_iota(i32, shape, dim)


def lane_take(x, idx):
    return jnp.take_along_axis(x, idx, axis=1, mode="promise_in_bounds")


def weigh_eight(stage, close):
    far = [x - 2.0 for x in close]
    total = [None] * 3
    for k in range(4):
        yy, xx = k >> 1, k & 1

        def load(c):
            return stage[c // 2, pl.ds(4 * yy + 2 * xx + c % 2, 8, stride=STEP), :]

        o = (far[0] if xx else close[0], far[1] if yy else close[1], close[2])
        d = [load(c) - o[c] for c in range(3)]
        dist = d[0] * d[0] + d[1] * d[1] + d[2] * d[2]
        weight = jnp.maximum(1.0 - dist, 0.0)
        for c in range(3):
            v = weight * load(3 + c)
            total[c] = v if k == 0 else total[c] + v
    return total


def edge_kernel(ph, counts, c63, c0, top, bottom, square, raw_x, raw_y, sem):
    reads = [pltpu.make_async_copy(ph.at[:, x], raw_x.at[k], sem.at[k]) for k, x in enumerate((CX - 1, 0))]
    reads += [pltpu.make_async_copy(ph.at[:, :, y, :], raw_y.at[k], sem.at[2 + k]) for k, y in enumerate((CY - 1, 0))]
    for read in reads:
        read.start()
    square[:CY, :CX] = counts[...].astype(f32)
    by_y = square[:CY, :].astype(i32)
    by_x = jnp.transpose(square[...])[:CX, :].astype(i32)
    for read in reads:
        read.wait()
    for k, (out, x) in enumerate(((c63, CX - 1), (c0, 0))):
        live = iota((CY, LANES), 1) < lane_take(by_y, jnp.full((CY, LANES), x, i32))
        for c in range(6):
            v = raw_x[k, c]
            out[c] = v if c < 3 else jnp.where(live, v, 0.0)
    for k, (out, y) in enumerate(((top, CY - 1), (bottom, 0))):
        live = iota((CX, LANES), 1) < lane_take(by_x, jnp.full((CX, LANES), y, i32))
        for c in range(6):
            v = raw_y[k, c]
            out[c] = v if c < 3 else jnp.where(live, v, 0.0)


def prep_kernel(blocks, offs, pix, tile_slot, flat, rel, owner, rank, target, points, places, sb, so, where):
    for k in range(4):
        for r in range(ROWS):
            sb[k, r : r + 1, :] = blocks[k : k + 1, r * LANES : (r + 1) * LANES]
    for c in range(3):
        for r in range(ROWS):
            so[c, r : r + 1, :] = offs[c : c + 1, r * LANES : (r + 1) * LANES]
    fx, fy = lax.axis_index("bx") * CX, lax.axis_index("by") * CY
    lx = [((sb[k] >> 8) - fx + 1) & (NXC - 1) for k in range(4)]
    ly = [((sb[k] & (NYC - 1)) - fy + 1) & (NYC - 1) for k in range(4)]
    qx = jnp.minimum(jnp.minimum(lx[0], lx[1]), jnp.minimum(lx[2], lx[3]))
    qy = jnp.minimum(jnp.minimum(ly[0], ly[1]), jnp.minimum(ly[2], ly[3]))
    at = qx * PAIR + qy * 4
    at = jnp.where(qy == CY, -1 - (2 * EDGE_X + EDGE_Y + 8 * qx), at)
    at = jnp.where(qy == 0, -1 - (2 * EDGE_X + 8 * qx), at)
    at = jnp.where(qx == CX, -1 - (EDGE_X + 4 * qy), at)
    at = jnp.where(qx == 0, -1 - 4 * qy, at)
    flat[...] = jnp.maximum(at, 0)
    rel[0] = 2.0 * (so[0] + (lx[0] - qx).astype(f32))
    rel[1] = 2.0 * (so[1] + (ly[0] - qy).astype(f32))
    rel[2] = 2.0 * so[2]
    for i in range(ROWS // 8):
        p = pix[8 * i : 8 * i + 8, :]
        tile = p >> 8
        low, high = tile & (LANES - 1), tile >> 7
        slot = jnp.zeros((8, LANES), i32)
        for t in range(8):
            row = jnp.broadcast_to(tile_slot[t : t + 1, :], (8, LANES))
            slot = jnp.where(high == t, lane_take(row, low), slot)
        owner[8 * i : 8 * i + 8, :] = slot >> 3
        target[8 * i : 8 * i + 8, :] = (slot & 7) * 256 + (p & 255)
    sub = iota((OWNERS, LANES), 0)
    upper = (iota((LANES, 2 * LANES), 0) <= iota((LANES, 2 * LANES), 1)).astype(f32).astype(bf16)

    def ranks(r, seen):
        hit = sub == jnp.broadcast_to(owner[pl.ds(r, 1), :], (OWNERS, LANES))
        tally = jnp.dot(jnp.where(hit, 1.0, 0.0).astype(bf16), upper, preferred_element_type=f32)
        rank[pl.ds(r, 1), :] = (
            jnp.sum(jnp.where(hit, tally[:, :LANES] + seen, 0.0), axis=0, keepdims=True) - 1.0
        ).astype(i32)
        return seen + tally[:, LANES:]

    lax.fori_loop(0, ROWS, ranks, jnp.zeros((OWNERS, LANES), f32), unroll=32)
    outside = at < 0
    tally = jnp.dot(jnp.where(outside, 1.0, 0.0).astype(bf16), upper, preferred_element_type=f32)
    before = iota((ROWS, ROWS), 1) < iota((ROWS, ROWS), 0)
    ahead = jnp.dot(
        jnp.where(before, 1.0, 0.0).astype(bf16), tally[:, LANES:].astype(bf16), preferred_element_type=f32
    )
    count = (ahead + tally[:, LANES:])[ROWS - 1 :].astype(i32)
    where[0] = jnp.where(outside, (ahead + tally[:, :LANES] - 1.0).astype(i32), -1)
    where[1] = iota((ROWS, LANES), 0) * LANES + iota((ROWS, LANES), 1)
    where[2] = -1 - at
    low_sub = iota((LANES, 2 * LANES), 0)
    high_sub = iota((ROWS, 2 * LANES), 0)

    def collect(r, total):
        spot, point, place = [
            jnp.concatenate([where[k, pl.ds(2 * r, 1), :], where[k, pl.ds(2 * r + 1, 1), :]], axis=1)
            for k in range(3)
        ]
        low_hit = jnp.where(low_sub == (spot & (LANES - 1)), 1.0, 0.0).astype(bf16)
        hit = high_sub == (spot >> 7)
        parts = [(point >> 8), (point & 255), (place >> 8), (place & 255)]
        rows = jnp.concatenate([jnp.where(hit, x.astype(f32), 0.0) for x in parts], axis=0).astype(bf16)
        return total + lax.dot_general(rows, low_hit, NT, preferred_element_type=f32)

    found = lax.fori_loop(0, ROWS // 2, collect, jnp.zeros((4 * ROWS, LANES), f32), unroll=16).astype(i32)
    points[:ROWS] = found[:ROWS] * 256 + found[ROWS : 2 * ROWS]
    places[:ROWS] = found[2 * ROWS : 3 * ROWS] * 256 + found[3 * ROWS :]
    points[ROWS:] = jnp.broadcast_to(count, (8, LANES))
    places[ROWS:] = jnp.broadcast_to(count, (8, LANES))

def inner_kernel(photons, counts, flat, rel, sums, near, ph, table, square, stage_a, stage_b, psem, ssem, *start):
    read = pltpu.make_async_copy(photons, ph, psem)
    read.start()
    to_scalar = [pltpu.make_async_copy(flat.at[pl.ds(4 * s, 4)], start[s], ssem.at[s]) for s in range(8)]
    for copy in to_scalar:
        copy.start()
    parts = [[rel[c, pl.ds(v, 8, stride=4), :] for c in range(3)] for v in range(4)]

    def spread(lane, _):
        take = jnp.full((8, LANES), lane, i32)
        for v in range(4):
            for c in range(3):
                near[c, v * LANES + lane] = lane_take(parts[v][c], take)
        return 0

    lax.fori_loop(0, LANES, spread, 0, unroll=16)
    square[:CY, :CX] = counts[...].astype(f32)
    filled = square[:CY, :].astype(i32)
    lane = iota((CY, LANES), 1)

    def row(c, x, y, right):
        return x * PAIR + (c // 2) * TWO + y * 4 + 2 * right + c % 2

    def column(x, _):
        live = lane < lane_take(filled, jnp.full((CY, LANES), x, i32))
        for c in range(6):
            v = ph[c, x]
            v = v + v if c < 3 else jnp.where(live, v, 0.0)
            table[pl.ds(row(c, x + 1, 1, 0), CY, stride=4), :] = v
            table[pl.ds(row(c, x, 1, 1), CY, stride=4), :] = v
        return 0

    read.wait()
    lax.fori_loop(0, CX, column, 0, unroll=8)
    for copy in to_scalar:
        copy.wait()
    zero = lax.axis_index("bx") * 0

    def fetch(i, stage):
        for u in range(GROUPS):
            g = jnp.minimum(i * GROUPS + u, POINTS // 8 - 1)
            v, lane = g >> 7, g & (LANES - 1)
            for s in range(8):
                r = start[s][v, lane]
                for j in range(3):
                    stage[u, j, pl.ds(zero + STEP * s, 8), :] = table[pl.ds(r + j * TWO, 8), :]

    def weigh(i, stage):
        for u in range(GROUPS):
            total = weigh_eight(stage.at[u], [near[c, i * GROUPS + u] for c in range(3)])
            for c in range(3):
                sums[c, pl.ds(i * GROUPS + u, 8, stride=APART), :] = total[c]

    def step(i, _):
        weigh(2 * i, stage_a)
        fetch(2 * i + 1, stage_b)
        weigh(2 * i + 1, stage_b)
        fetch(2 * i + 2, stage_a)
        return 0

    fetch(0, stage_a)
    lax.fori_loop(0, POINTS // 16 // GROUPS, step, 0)


def outer_kernel(points, places, sums, near, alb, owner, rank, target, xm, xp, c0, c63, ym, yp, bottom, top,
                 send, edge, stage, close, rad):
    for c in range(6):
        scale = 2.0 if c < 3 else 1.0
        plane = (c // 2) * EDGE + c % 2
        for base, cols in ((0, ((xm, 0), (c0, 1))), (EDGE_X, ((c63, CX), (xp, CX + 1)))):
            for right, (col, x) in enumerate(cols):
                at = plane + base + 2 * right
                edge[pl.ds(at + 4, CY, stride=4), :] = col[c] * scale
                edge[at : at + 1, :] = ym[c, x : x + 1] * scale
                edge[at + 4 * EY - 4 : at + 4 * EY - 3, :] = yp[c, x : x + 1] * scale
        for base, lines in ((2 * EDGE_X, (ym, bottom)), (2 * EDGE_X + EDGE_Y, (top, yp))):
            for yy, line in enumerate(lines):
                for right in range(2):
                    at = plane + base + 4 * yy + 2 * right
                    edge[pl.ds(at, CX + 1, stride=8), :] = line[c, right : right + CX + 1] * scale
    sub = iota((8, LANES), 0)
    zero = lax.axis_index("bx") * 0
    count = points[ROWS, 0]

    def eight(i, stage, close):
        where = []
        for s in range(8):
            k = jnp.minimum(8 * i + s, count - 1)
            p, r = points[k >> 7, k & (LANES - 1)], places[k >> 7, k & (LANES - 1)]
            where.append((p >> 9) * APART + (p & 511))
            for c in range(3):
                close[c, s : s + 1, :] = near[c, p & 511, pl.ds(p >> 9, 1), :]
            for j in range(3):
                stage[j, pl.ds(zero + STEP * s, 8), :] = edge[pl.ds(r + j * EDGE, 8), :]
        total = weigh_eight(stage, [close[c] for c in range(3)])
        for c in range(3):
            for s in range(8):
                sums[c, pl.ds(where[s], 1), :] = total[c][s : s + 1]

    def eights(i, _):
        for u in range(TOGETHER):
            eight(TOGETHER * i + u, stage.at[u], close.at[u])
        return 0

    lax.fori_loop(0, lax.div(count + 8 * TOGETHER - 1, 8 * TOGETHER), eights, 0)
    ones = jnp.ones((8, 2 * LANES), f32).astype(bf16)

    def lane_sums(r, _):
        for c in range(3):
            for k in range(2):
                line = 2 * r + k
                x = sums[c, pl.ds((line >> 2) * APART + (line & 3) * LANES, LANES), :]
                high = x.astype(bf16)
                low = (x - high.astype(f32)).astype(bf16)
                both = jnp.concatenate([high, low], axis=1)
                y = lax.dot_general(ones, both, NT, preferred_element_type=f32)
                rad[c, pl.ds(line, 1), :] = y[:1]
        return 0

    lax.fori_loop(0, ROWS // 2, lane_sums, 0, unroll=16)
    for c in range(3):
        for r in range(ROWS):
            rad[c, r : r + 1, :] = rad[c, r : r + 1, :] * alb[c : c + 1, r * LANES : (r + 1) * LANES]
    wide_sub = iota((OWNERS, 2 * LANES), 0)
    rank_sub = iota((CAP, 2 * LANES), 0)

    def two(ref, r):
        return jnp.concatenate([ref[pl.ds(2 * r, 1), :], ref[pl.ds(2 * r + 1, 1), :]], axis=1)

    def scatter(r, total):
        mine = jnp.where(wide_sub == two(owner, r), 1.0, 0.0).astype(bf16)
        hit = rank_sub == two(rank, r)
        where = two(target, r)
        vals = [two(rad.at[c], r) for c in range(3)]
        high = [x.astype(bf16).astype(f32) for x in vals]
        low = [x - h for x, h in zip(vals, high)]
        high.append((where & ~255).astype(f32))
        low.append((where & 255).astype(f32))
        for part in (high, low):
            rows = jnp.concatenate([jnp.where(hit, x, 0.0) for x in part], axis=0).astype(bf16)
            total = total + lax.dot_general(mine, rows, NT, preferred_element_type=f32)
        return total

    send[:, 0, :] = lax.fori_loop(0, ROWS // 2, scatter, jnp.zeros((OWNERS, 4 * CAP), f32), unroll=16)


def film_kernel(got, film, flipped, total):
    for j in range(3):
        flipped[LANES * j : LANES * j + LANES, :] = jnp.transpose(got[:, 0, LANES * j : LANES * j + LANES])
    lo_sub = iota((LANES, 2 * LANES), 0)
    hi_sub = iota((16, 2 * LANES), 0)

    def two(row):
        return jnp.concatenate(
            [flipped[pl.ds(row, 1), :], flipped[pl.ds(row + CAP // 2, 1), :]], axis=1
        )

    def step(k, acc):
        where = two(3 * CAP + k).astype(i32)
        low_hit = jnp.where(lo_sub == (where & 127), 1.0, 0.0).astype(bf16)
        hit = hi_sub == (where >> 7)
        high, low = [], []
        for c in range(3):
            x = two(c * CAP + k)
            h = x.astype(bf16).astype(f32)
            high.append(jnp.where(hit, h, 0.0))
            low.append(jnp.where(hit, x - h, 0.0))
        rows = jnp.concatenate(high + low, axis=0).astype(bf16)
        return acc + lax.dot_general(rows, low_hit, NT, preferred_element_type=f32)

    acc = lax.fori_loop(0, CAP // 2, step, jnp.zeros((96, LANES), f32), unroll=48)
    total[...] = acc[:48] + acc[48:]
    for c in range(3):
        film[c, :, :LANES] = total[pl.ds(16 * c, 8, stride=2), :]
        film[c, :, LANES:] = total[pl.ds(16 * c + 1, 8, stride=2), :]


def shift(x, axis, by):
    n = lax.axis_size(axis)
    return lax.ppermute(x, axis, [(i, (i + by) % n) for i in range(n)])


def per_device(photon_data, block_counts, gather_offsets, gather_blocks, albedo, gather_pixels, tile_slot):
    small_i = jax.ShapeDtypeStruct((ROWS, LANES), i32)
    listed = jax.ShapeDtypeStruct((LIST, LANES), i32)
    column, line = jax.ShapeDtypeStruct((6, CY, LANES), f32), jax.ShapeDtypeStruct((6, CX, LANES), f32)
    counts = block_counts.T
    c63, c0, top, bottom = pl.pallas_call(
        edge_kernel,
        in_specs=[HBM, VMEM],
        out_specs=[VMEM] * 4,
        out_shape=[column, column, line, line],
        scratch_shapes=[
            pltpu.VMEM((LANES, LANES), f32),
            pltpu.VMEM((2, 6, CY, LANES), f32),
            pltpu.VMEM((2, 6, CX, LANES), f32),
            pltpu.SemaphoreType.DMA((4,)),
        ],
        compiler_params=params(60),
        name="edges",
    )(photon_data, counts)
    xm, xp = shift(c63, "bx", 1), shift(c0, "bx", -1)
    flat, rel, owner, rank, target, points, places = pl.pallas_call(
        prep_kernel,
        in_specs=[VMEM] * 4,
        out_specs=[VMEM] * 7,
        out_shape=[small_i, jax.ShapeDtypeStruct((3, ROWS, LANES), f32), small_i, small_i, small_i, listed, listed],
        scratch_shapes=[
            pltpu.VMEM((4, ROWS, LANES), i32),
            pltpu.VMEM((3, ROWS, LANES), f32),
            pltpu.VMEM((3, ROWS, LANES), i32),
        ],
        compiler_params=params(16),
        cost_estimate=pl.CostEstimate(flops=4000000000, bytes_accessed=40000000, transcendentals=0),
        name="prep",
    )(gather_blocks, gather_offsets, gather_pixels.reshape(ROWS, LANES), tile_slot.reshape(8, LANES))
    top, bottom, rank = lax.optimization_barrier((top, bottom, rank))
    top = jnp.concatenate([xm[:, -1:], top, xp[:, -1:]], axis=1)
    bottom = jnp.concatenate([xm[:, :1], bottom, xp[:, :1]], axis=1)
    ym, yp = shift(top, "by", 1), shift(bottom, "by", -1)
    sums, near = pl.pallas_call(
        inner_kernel,
        in_specs=[HBM] + [VMEM] * 3,
        out_specs=[VMEM] * 2,
        out_shape=[
            jax.ShapeDtypeStruct((3, 8 * APART, LANES), f32),
            jax.ShapeDtypeStruct((3, POINTS // 8, 8, LANES), f32),
        ],
        scratch_shapes=[
            pltpu.VMEM((6, CX, CY, LANES), f32),
            pltpu.VMEM((TABLE_ROWS, LANES), f32),
            pltpu.VMEM((CY, LANES), f32),
            pltpu.VMEM((GROUPS, 3, 8 * STEP + 8, LANES), f32),
            pltpu.VMEM((GROUPS, 3, 8 * STEP + 8, LANES), f32),
            pltpu.SemaphoreType.DMA,
            pltpu.SemaphoreType.DMA((8,)),
        ]
        + [pltpu.SMEM((4, LANES), i32)] * 8,
        compiler_params=params(34),
        cost_estimate=pl.CostEstimate(flops=60_000_000, bytes_accessed=7_000_000, transcendentals=0),
        name="inner",
    )(photon_data, counts, flat, rel)
    send = pl.pallas_call(
        outer_kernel,
        in_specs=[SMEM] * 2 + [VMEM] * 14,
        out_specs=VMEM,
        out_shape=jax.ShapeDtypeStruct((OWNERS, 1, 4 * CAP), f32),
        scratch_shapes=[
            pltpu.VMEM((3 * EDGE + 64, LANES), f32),
            pltpu.VMEM((TOGETHER, 3, 8 * STEP + 8, LANES), f32),
            pltpu.VMEM((TOGETHER, 3, 8, LANES), f32),
            pltpu.VMEM((3, ROWS, LANES), f32),
        ],
        compiler_params=params(16),
        name="outer",
    )(points, places, sums, near, albedo, owner, rank, target, xm, xp, c0, c63, ym, yp, bottom, top)
    got = lax.all_to_all(send, AXES, 0, 0, tiled=True)
    return pl.pallas_call(
        film_kernel,
        in_specs=[VMEM],
        out_specs=VMEM,
        out_shape=jax.ShapeDtypeStruct((3, 8, 256), f32),
        scratch_shapes=[pltpu.VMEM((4 * CAP, LANES), f32), pltpu.VMEM((48, LANES), f32)],
        compiler_params=params(16),
        name="film",
    )(got)


def solution(mesh):
    in_specs = (P(None, "bx", "by", None), P("bx", "by"), P(None, AXES), P(None, AXES), P(None, AXES), P(AXES), P())
    return jax.shard_map(per_device, mesh=mesh, in_specs=in_specs, out_specs=P(None, AXES, None), check_vma=False)
```

```python
import jax
import jax.numpy as jnp
from jax import lax
from jax.experimental import pallas as pl
from jax.experimental.pallas import tpu as pltpu
from jax.sharding import PartitionSpec as P

AXES = ("bx", "by")
CX, CY = 64, 32
EX, EY = CX + 2, CY + 2
NXC, NYC = 1024, 256
LANES = 128
POINTS = 4096
ROWS = POINTS // LANES
CAP = 96
OWNERS = 128
TWO = 4 * EY
PAIR = 3 * TWO
TABLE_ROWS = (CX + 1) * PAIR
APART = 513
EDGE_X, EDGE_Y = 4 * EY, 8 * (CX + 1)
EDGE = 2 * EDGE_X + 2 * EDGE_Y
LIST = ROWS + 8
STEP = 9
TOGETHER = 8
GROUPS = 4
i32, f32, bf16 = jnp.int32, jnp.float32, jnp.bfloat16
VMEM = pl.BlockSpec(memory_space=pltpu.VMEM)
SMEM = pl.BlockSpec(memory_space=pltpu.SMEM)
NT = (((1,), (1,)), ((), ()))


HBM = pl.BlockSpec(memory_space=pltpu.HBM)


def params(mib):
    return pltpu.CompilerParams(vmem_limit_bytes=int(mib * 1024 * 1024))


def iota(shape, dim):
    return lax.broadcasted_iota(i32, shape, dim)


def lane_take(x, idx):
    return jnp.take_along_axis(x, idx, axis=1, mode="promise_in_bounds")


def weigh_eight(stage, close):
    far = [x - 2.0 for x in close]
    total = [None] * 3
    for k in range(4):
        yy, xx = k >> 1, k & 1

        def load(c):
            return stage[c // 2, pl.ds(4 * yy + 2 * xx + c % 2, 8, stride=STEP), :]

        o = (far[0] if xx else close[0], far[1] if yy else close[1], close[2])
        d = [load(c) - o[c] for c in range(3)]
        dist = d[0] * d[0] + d[1] * d[1] + d[2] * d[2]
        weight = jnp.maximum(1.0 - dist, 0.0)
        for c in range(3):
            v = weight * load(3 + c)
            total[c] = v if k == 0 else total[c] + v
    return total


def edge_kernel(ph, counts, c63, c0, top, bottom, square, raw_x, raw_y, sem):
    reads = [pltpu.make_async_copy(ph.at[:, x], raw_x.at[k], sem.at[k]) for k, x in enumerate((CX - 1, 0))]
    reads += [pltpu.make_async_copy(ph.at[:, :, y, :], raw_y.at[k], sem.at[2 + k]) for k, y in enumerate((CY - 1, 0))]
    for read in reads:
        read.start()
    square[:CY, :CX] = counts[...].astype(f32)
    by_y = square[:CY, :].astype(i32)
    by_x = jnp.transpose(square[...])[:CX, :].astype(i32)
    for read in reads:
        read.wait()
    for k, (out, x) in enumerate(((c63, CX - 1), (c0, 0))):
        live = iota((CY, LANES), 1) < lane_take(by_y, jnp.full((CY, LANES), x, i32))
        for c in range(6):
            v = raw_x[k, c]
            out[c] = v if c < 3 else jnp.where(live, v, 0.0)
    for k, (out, y) in enumerate(((top, CY - 1), (bottom, 0))):
        live = iota((CX, LANES), 1) < lane_take(by_x, jnp.full((CX, LANES), y, i32))
        for c in range(6):
            v = raw_y[k, c]
            out[c] = v if c < 3 else jnp.where(live, v, 0.0)


def prep_kernel(blocks, offs, pix, tile_slot, flat, rel, owner, rank, target, points, places, sb, so, where):
    for k in range(4):
        for r in range(ROWS):
            sb[k, r : r + 1, :] = blocks[k : k + 1, r * LANES : (r + 1) * LANES]
    for c in range(3):
        for r in range(ROWS):
            so[c, r : r + 1, :] = offs[c : c + 1, r * LANES : (r + 1) * LANES]
    fx, fy = lax.axis_index("bx") * CX, lax.axis_index("by") * CY
    lx = [((sb[k] >> 8) - fx + 1) & (NXC - 1) for k in range(4)]
    ly = [((sb[k] & (NYC - 1)) - fy + 1) & (NYC - 1) for k in range(4)]
    qx = jnp.minimum(jnp.minimum(lx[0], lx[1]), jnp.minimum(lx[2], lx[3]))
    qy = jnp.minimum(jnp.minimum(ly[0], ly[1]), jnp.minimum(ly[2], ly[3]))
    at = qx * PAIR + qy * 4
    at = jnp.where(qy == CY, -1 - (2 * EDGE_X + EDGE_Y + 8 * qx), at)
    at = jnp.where(qy == 0, -1 - (2 * EDGE_X + 8 * qx), at)
    at = jnp.where(qx == CX, -1 - (EDGE_X + 4 * qy), at)
    at = jnp.where(qx == 0, -1 - 4 * qy, at)
    flat[...] = jnp.maximum(at, 0)
    rel[0] = 2.0 * (so[0] + (lx[0] - qx).astype(f32))
    rel[1] = 2.0 * (so[1] + (ly[0] - qy).astype(f32))
    rel[2] = 2.0 * so[2]
    for i in range(ROWS // 8):
        p = pix[8 * i : 8 * i + 8, :]
        tile = p >> 8
        low, high = tile & (LANES - 1), tile >> 7
        slot = jnp.zeros((8, LANES), i32)
        for t in range(8):
            row = jnp.broadcast_to(tile_slot[t : t + 1, :], (8, LANES))
            slot = jnp.where(high == t, lane_take(row, low), slot)
        owner[8 * i : 8 * i + 8, :] = slot >> 3
        target[8 * i : 8 * i + 8, :] = (slot & 7) * 256 + (p & 255)
    sub = iota((OWNERS, LANES), 0)
    upper = (iota((LANES, 2 * LANES), 0) <= iota((LANES, 2 * LANES), 1)).astype(f32).astype(bf16)

    def ranks(r, seen):
        hit = sub == jnp.broadcast_to(owner[pl.ds(r, 1), :], (OWNERS, LANES))
        tally = jnp.dot(jnp.where(hit, 1.0, 0.0).astype(bf16), upper, preferred_element_type=f32)
        rank[pl.ds(r, 1), :] = (
            jnp.sum(jnp.where(hit, tally[:, :LANES] + seen, 0.0), axis=0, keepdims=True) - 1.0
        ).astype(i32)
        return seen + tally[:, LANES:]

    lax.fori_loop(0, ROWS, ranks, jnp.zeros((OWNERS, LANES), f32), unroll=32)
    outside = at < 0
    tally = jnp.dot(jnp.where(outside, 1.0, 0.0).astype(bf16), upper, preferred_element_type=f32)
    before = iota((ROWS, ROWS), 1) < iota((ROWS, ROWS), 0)
    ahead = jnp.dot(
        jnp.where(before, 1.0, 0.0).astype(bf16), tally[:, LANES:].astype(bf16), preferred_element_type=f32
    )
    count = (ahead + tally[:, LANES:])[ROWS - 1 :].astype(i32)
    where[0] = jnp.where(outside, (ahead + tally[:, :LANES] - 1.0).astype(i32), -1)
    where[1] = iota((ROWS, LANES), 0) * LANES + iota((ROWS, LANES), 1)
    where[2] = -1 - at
    low_sub = iota((LANES, 2 * LANES), 0)
    high_sub = iota((ROWS, 2 * LANES), 0)

    def collect(r, total):
        spot, point, place = [
            jnp.concatenate([where[k, pl.ds(2 * r, 1), :], where[k, pl.ds(2 * r + 1, 1), :]], axis=1)
            for k in range(3)
        ]
        low_hit = jnp.where(low_sub == (spot & (LANES - 1)), 1.0, 0.0).astype(bf16)
        hit = high_sub == (spot >> 7)
        parts = [(point >> 8), (point & 255), (place >> 8), (place & 255)]
        rows = jnp.concatenate([jnp.where(hit, x.astype(f32), 0.0) for x in parts], axis=0).astype(bf16)
        return total + lax.dot_general(rows, low_hit, NT, preferred_element_type=f32)

    found = lax.fori_loop(0, ROWS // 2, collect, jnp.zeros((4 * ROWS, LANES), f32), unroll=16).astype(i32)
    points[:ROWS] = found[:ROWS] * 256 + found[ROWS : 2 * ROWS]
    places[:ROWS] = found[2 * ROWS : 3 * ROWS] * 256 + found[3 * ROWS :]
    points[ROWS:] = jnp.broadcast_to(count, (8, LANES))
    places[ROWS:] = jnp.broadcast_to(count, (8, LANES))

def inner_kernel(photons, counts, flat, rel, sums, near, ph, table, square, stage_a, stage_b, psem, ssem, *start):
    read = pltpu.make_async_copy(photons, ph, psem)
    read.start()
    to_scalar = [pltpu.make_async_copy(flat.at[pl.ds(4 * s, 4)], start[s], ssem.at[s]) for s in range(8)]
    for copy in to_scalar:
        copy.start()
    parts = [[rel[c, pl.ds(v, 8, stride=4), :] for c in range(3)] for v in range(4)]

    def spread(lane, _):
        take = jnp.full((8, LANES), lane, i32)
        for v in range(4):
            for c in range(3):
                near[c, v * LANES + lane] = lane_take(parts[v][c], take)
        return 0

    lax.fori_loop(0, LANES, spread, 0, unroll=32)
    square[:CY, :CX] = counts[...].astype(f32)
    filled = square[:CY, :].astype(i32)
    lane = iota((CY, LANES), 1)

    def row(c, x, y, right):
        return x * PAIR + (c // 2) * TWO + y * 4 + 2 * right + c % 2

    def column(x, _):
        live = lane < lane_take(filled, jnp.full((CY, LANES), x, i32))
        for c in range(6):
            v = ph[c, x]
            v = v + v if c < 3 else jnp.where(live, v, 0.0)
            table[pl.ds(row(c, x + 1, 1, 0), CY, stride=4), :] = v
            table[pl.ds(row(c, x, 1, 1), CY, stride=4), :] = v
        return 0

    read.wait()
    lax.fori_loop(0, CX, column, 0, unroll=16)
    for copy in to_scalar:
        copy.wait()
    zero = lax.axis_index("bx") * 0

    def fetch(i, stage):
        for u in range(GROUPS):
            g = jnp.minimum(i * GROUPS + u, POINTS // 8 - 1)
            v, lane = g >> 7, g & (LANES - 1)
            for s in range(8):
                r = start[s][v, lane]
                for j in range(3):
                    stage[u, j, pl.ds(zero + STEP * s, 8), :] = table[pl.ds(r + j * TWO, 8), :]

    def weigh(i, stage):
        for u in range(GROUPS):
            total = weigh_eight(stage.at[u], [near[c, i * GROUPS + u] for c in range(3)])
            for c in range(3):
                sums[c, pl.ds(i * GROUPS + u, 8, stride=APART), :] = total[c]

    def step(i, _):
        weigh(2 * i, stage_a)
        fetch(2 * i + 1, stage_b)
        weigh(2 * i + 1, stage_b)
        fetch(2 * i + 2, stage_a)
        return 0

    fetch(0, stage_a)
    lax.fori_loop(0, POINTS // 16 // GROUPS, step, 0)


def outer_kernel(points, places, sums, near, alb, owner, rank, target, xm, xp, c0, c63, ym, yp, bottom, top,
                 send, edge, stage, close, rad):
    for c in range(6):
        scale = 2.0 if c < 3 else 1.0
        plane = (c // 2) * EDGE + c % 2
        for base, cols in ((0, ((xm, 0), (c0, 1))), (EDGE_X, ((c63, CX), (xp, CX + 1)))):
            for right, (col, x) in enumerate(cols):
                at = plane + base + 2 * right
                edge[pl.ds(at + 4, CY, stride=4), :] = col[c] * scale
                edge[at : at + 1, :] = ym[c, x : x + 1] * scale
                edge[at + 4 * EY - 4 : at + 4 * EY - 3, :] = yp[c, x : x + 1] * scale
        for base, lines in ((2 * EDGE_X, (ym, bottom)), (2 * EDGE_X + EDGE_Y, (top, yp))):
            for yy, line in enumerate(lines):
                for right in range(2):
                    at = plane + base + 4 * yy + 2 * right
                    edge[pl.ds(at, CX + 1, stride=8), :] = line[c, right : right + CX + 1] * scale
    sub = iota((8, LANES), 0)
    zero = lax.axis_index("bx") * 0
    count = points[ROWS, 0]

    def eight(i, stage, close):
        where = []
        for s in range(8):
            k = jnp.minimum(8 * i + s, count - 1)
            p, r = points[k >> 7, k & (LANES - 1)], places[k >> 7, k & (LANES - 1)]
            where.append((p >> 9) * APART + (p & 511))
            for c in range(3):
                close[c, s : s + 1, :] = near[c, p & 511, pl.ds(p >> 9, 1), :]
            for j in range(3):
                stage[j, pl.ds(zero + STEP * s, 8), :] = edge[pl.ds(r + j * EDGE, 8), :]
        total = weigh_eight(stage, [close[c] for c in range(3)])
        for c in range(3):
            for s in range(8):
                sums[c, pl.ds(where[s], 1), :] = total[c][s : s + 1]

    def eights(i, _):
        for u in range(TOGETHER):
            eight(TOGETHER * i + u, stage.at[u], close.at[u])
        return 0

    lax.fori_loop(0, lax.div(count + 8 * TOGETHER - 1, 8 * TOGETHER), eights, 0)
    ones = jnp.ones((8, 2 * LANES), f32).astype(bf16)

    def lane_sums(r, _):
        for c in range(3):
            for k in range(2):
                line = 2 * r + k
                x = sums[c, pl.ds((line >> 2) * APART + (line & 3) * LANES, LANES), :]
                high = x.astype(bf16)
                low = (x - high.astype(f32)).astype(bf16)
                both = jnp.concatenate([high, low], axis=1)
                y = lax.dot_general(ones, both, NT, preferred_element_type=f32)
                rad[c, pl.ds(line, 1), :] = y[:1]
        return 0

    lax.fori_loop(0, ROWS // 2, lane_sums, 0, unroll=16)
    for c in range(3):
        for r in range(ROWS):
            rad[c, r : r + 1, :] = rad[c, r : r + 1, :] * alb[c : c + 1, r * LANES : (r + 1) * LANES]
    wide_sub = iota((OWNERS, 2 * LANES), 0)
    rank_sub = iota((CAP, 2 * LANES), 0)

    def two(ref, r):
        return jnp.concatenate([ref[pl.ds(2 * r, 1), :], ref[pl.ds(2 * r + 1, 1), :]], axis=1)

    def scatter(r, total):
        mine = jnp.where(wide_sub == two(owner, r), 1.0, 0.0).astype(bf16)
        hit = rank_sub == two(rank, r)
        where = two(target, r)
        vals = [two(rad.at[c], r) for c in range(3)]
        high = [x.astype(bf16).astype(f32) for x in vals]
        low = [x - h for x, h in zip(vals, high)]
        high.append((where & ~255).astype(f32))
        low.append((where & 255).astype(f32))
        for part in (high, low):
            rows = jnp.concatenate([jnp.where(hit, x, 0.0) for x in part], axis=0).astype(bf16)
            total = total + lax.dot_general(mine, rows, NT, preferred_element_type=f32)
        return total

    send[:, 0, :] = lax.fori_loop(0, ROWS // 2, scatter, jnp.zeros((OWNERS, 4 * CAP), f32), unroll=16)


def film_kernel(got, film, flipped, total):
    for j in range(3):
        flipped[LANES * j : LANES * j + LANES, :] = jnp.transpose(got[:, 0, LANES * j : LANES * j + LANES])
    lo_sub = iota((LANES, 2 * LANES), 0)
    hi_sub = iota((16, 2 * LANES), 0)

    def two(row):
        return jnp.concatenate(
            [flipped[pl.ds(row, 1), :], flipped[pl.ds(row + CAP // 2, 1), :]], axis=1
        )

    def step(k, acc):
        where = two(3 * CAP + k).astype(i32)
        low_hit = jnp.where(lo_sub == (where & 127), 1.0, 0.0).astype(bf16)
        hit = hi_sub == (where >> 7)
        high, low = [], []
        for c in range(3):
            x = two(c * CAP + k)
            h = x.astype(bf16).astype(f32)
            high.append(jnp.where(hit, h, 0.0))
            low.append(jnp.where(hit, x - h, 0.0))
        rows = jnp.concatenate(high + low, axis=0).astype(bf16)
        return acc + lax.dot_general(rows, low_hit, NT, preferred_element_type=f32)

    acc = lax.fori_loop(0, CAP // 2, step, jnp.zeros((96, LANES), f32), unroll=48)
    total[...] = acc[:48] + acc[48:]
    for c in range(3):
        film[c, :, :LANES] = total[pl.ds(16 * c, 8, stride=2), :]
        film[c, :, LANES:] = total[pl.ds(16 * c + 1, 8, stride=2), :]


def shift(x, axis, by):
    n = lax.axis_size(axis)
    return lax.ppermute(x, axis, [(i, (i + by) % n) for i in range(n)])


def per_device(photon_data, block_counts, gather_offsets, gather_blocks, albedo, gather_pixels, tile_slot):
    small_i = jax.ShapeDtypeStruct((ROWS, LANES), i32)
    listed = jax.ShapeDtypeStruct((LIST, LANES), i32)
    column, line = jax.ShapeDtypeStruct((6, CY, LANES), f32), jax.ShapeDtypeStruct((6, CX, LANES), f32)
    counts = block_counts.T
    c63, c0, top, bottom = pl.pallas_call(
        edge_kernel,
        in_specs=[HBM, VMEM],
        out_specs=[VMEM] * 4,
        out_shape=[column, column, line, line],
        scratch_shapes=[
            pltpu.VMEM((LANES, LANES), f32),
            pltpu.VMEM((2, 6, CY, LANES), f32),
            pltpu.VMEM((2, 6, CX, LANES), f32),
            pltpu.SemaphoreType.DMA((4,)),
        ],
        compiler_params=params(60),
        name="edges",
    )(photon_data, counts)
    xm, xp = shift(c63, "bx", 1), shift(c0, "bx", -1)
    flat, rel, owner, rank, target, points, places = pl.pallas_call(
        prep_kernel,
        in_specs=[VMEM] * 4,
        out_specs=[VMEM] * 7,
        out_shape=[small_i, jax.ShapeDtypeStruct((3, ROWS, LANES), f32), small_i, small_i, small_i, listed, listed],
        scratch_shapes=[
            pltpu.VMEM((4, ROWS, LANES), i32),
            pltpu.VMEM((3, ROWS, LANES), f32),
            pltpu.VMEM((3, ROWS, LANES), i32),
        ],
        compiler_params=params(16),
        cost_estimate=pl.CostEstimate(flops=4000000000, bytes_accessed=40000000, transcendentals=0),
        name="prep",
    )(gather_blocks, gather_offsets, gather_pixels.reshape(ROWS, LANES), tile_slot.reshape(8, LANES))
    top, bottom, rank = lax.optimization_barrier((top, bottom, rank))
    top = jnp.concatenate([xm[:, -1:], top, xp[:, -1:]], axis=1)
    bottom = jnp.concatenate([xm[:, :1], bottom, xp[:, :1]], axis=1)
    ym, yp = shift(top, "by", 1), shift(bottom, "by", -1)
    sums, near = pl.pallas_call(
        inner_kernel,
        in_specs=[HBM] + [VMEM] * 3,
        out_specs=[VMEM] * 2,
        out_shape=[
            jax.ShapeDtypeStruct((3, 8 * APART, LANES), f32),
            jax.ShapeDtypeStruct((3, POINTS // 8, 8, LANES), f32),
        ],
        scratch_shapes=[
            pltpu.VMEM((6, CX, CY, LANES), f32),
            pltpu.VMEM((TABLE_ROWS, LANES), f32),
            pltpu.VMEM((CY, LANES), f32),
            pltpu.VMEM((GROUPS, 3, 8 * STEP + 8, LANES), f32),
            pltpu.VMEM((GROUPS, 3, 8 * STEP + 8, LANES), f32),
            pltpu.SemaphoreType.DMA,
            pltpu.SemaphoreType.DMA((8,)),
        ]
        + [pltpu.SMEM((4, LANES), i32)] * 8,
        compiler_params=params(34),
        cost_estimate=pl.CostEstimate(flops=60_000_000, bytes_accessed=7_000_000, transcendentals=0),
        name="inner",
    )(photon_data, counts, flat, rel)
    send = pl.pallas_call(
        outer_kernel,
        in_specs=[SMEM] * 2 + [VMEM] * 14,
        out_specs=VMEM,
        out_shape=jax.ShapeDtypeStruct((OWNERS, 1, 4 * CAP), f32),
        scratch_shapes=[
            pltpu.VMEM((3 * EDGE + 64, LANES), f32),
            pltpu.VMEM((TOGETHER, 3, 8 * STEP + 8, LANES), f32),
            pltpu.VMEM((TOGETHER, 3, 8, LANES), f32),
            pltpu.VMEM((3, ROWS, LANES), f32),
        ],
        compiler_params=params(16),
        name="outer",
    )(points, places, sums, near, albedo, owner, rank, target, xm, xp, c0, c63, ym, yp, bottom, top)
    got = lax.all_to_all(send, AXES, 0, 0, tiled=True)
    return pl.pallas_call(
        film_kernel,
        in_specs=[VMEM],
        out_specs=VMEM,
        out_shape=jax.ShapeDtypeStruct((3, 8, 256), f32),
        scratch_shapes=[pltpu.VMEM((4 * CAP, LANES), f32), pltpu.VMEM((48, LANES), f32)],
        compiler_params=params(16),
        name="film",
    )(got)


def solution(mesh):
    in_specs = (P(None, "bx", "by", None), P("bx", "by"), P(None, AXES), P(None, AXES), P(None, AXES), P(AXES), P())
    return jax.shard_map(per_device, mesh=mesh, in_specs=in_specs, out_specs=P(None, AXES, None), check_vma=False)
```

```python
import jax
import jax.numpy as jnp
from jax import lax
from jax.experimental import pallas as pl
from jax.experimental.pallas import tpu as pltpu
from jax.sharding import PartitionSpec as P

AXES = ("bx", "by")
CX, CY = 64, 32
EX, EY = CX + 2, CY + 2
NXC, NYC = 1024, 256
LANES = 128
POINTS = 4096
ROWS = POINTS // LANES
CAP = 96
OWNERS = 128
TWO = 4 * EY
PAIR = 3 * TWO
TABLE_ROWS = (CX + 1) * PAIR
APART = 513
EDGE_X, EDGE_Y = 4 * EY, 8 * (CX + 1)
EDGE = 2 * EDGE_X + 2 * EDGE_Y
LIST = ROWS + 8
STEP = 9
TOGETHER = 8
GROUPS = 4
i32, f32, bf16 = jnp.int32, jnp.float32, jnp.bfloat16
VMEM = pl.BlockSpec(memory_space=pltpu.VMEM)
SMEM = pl.BlockSpec(memory_space=pltpu.SMEM)
NT = (((1,), (1,)), ((), ()))


HBM = pl.BlockSpec(memory_space=pltpu.HBM)


def params(mib):
    return pltpu.CompilerParams(vmem_limit_bytes=int(mib * 1024 * 1024))


def iota(shape, dim):
    return lax.broadcasted_iota(i32, shape, dim)


def lane_take(x, idx):
    return jnp.take_along_axis(x, idx, axis=1, mode="promise_in_bounds")


def weigh_eight(stage, close):
    far = [x - 2.0 for x in close]
    total = [None] * 3
    for k in range(4):
        yy, xx = k >> 1, k & 1

        def load(c):
            return stage[c // 2, pl.ds(4 * yy + 2 * xx + c % 2, 8, stride=STEP), :]

        o = (far[0] if xx else close[0], far[1] if yy else close[1], close[2])
        d = [load(c) - o[c] for c in range(3)]
        dist = d[0] * d[0] + d[1] * d[1] + d[2] * d[2]
        weight = jnp.maximum(1.0 - dist, 0.0)
        for c in range(3):
            v = weight * load(3 + c)
            total[c] = v if k == 0 else total[c] + v
    return total


def edge_kernel(ph, counts, c63, c0, top, bottom, square, raw_x, raw_y, sem):
    reads = [pltpu.make_async_copy(ph.at[:, x], raw_x.at[k], sem.at[k]) for k, x in enumerate((CX - 1, 0))]
    reads += [pltpu.make_async_copy(ph.at[:, :, y, :], raw_y.at[k], sem.at[2 + k]) for k, y in enumerate((CY - 1, 0))]
    for read in reads:
        read.start()
    square[:CY, :CX] = counts[...].astype(f32)
    by_y = square[:CY, :].astype(i32)
    by_x = jnp.transpose(square[...])[:CX, :].astype(i32)
    for read in reads:
        read.wait()
    for k, (out, x) in enumerate(((c63, CX - 1), (c0, 0))):
        live = iota((CY, LANES), 1) < lane_take(by_y, jnp.full((CY, LANES), x, i32))
        for c in range(6):
            v = raw_x[k, c]
            out[c] = v if c < 3 else jnp.where(live, v, 0.0)
    for k, (out, y) in enumerate(((top, CY - 1), (bottom, 0))):
        live = iota((CX, LANES), 1) < lane_take(by_x, jnp.full((CX, LANES), y, i32))
        for c in range(6):
            v = raw_y[k, c]
            out[c] = v if c < 3 else jnp.where(live, v, 0.0)


def prep_kernel(blocks, offs, pix, tile_slot, flat, rel, owner, rank, target, points, places, sb, so, where):
    for k in range(4):
        for r in range(ROWS):
            sb[k, r : r + 1, :] = blocks[k : k + 1, r * LANES : (r + 1) * LANES]
    for c in range(3):
        for r in range(ROWS):
            so[c, r : r + 1, :] = offs[c : c + 1, r * LANES : (r + 1) * LANES]
    fx, fy = lax.axis_index("bx") * CX, lax.axis_index("by") * CY
    lx = [((sb[k] >> 8) - fx + 1) & (NXC - 1) for k in range(4)]
    ly = [((sb[k] & (NYC - 1)) - fy + 1) & (NYC - 1) for k in range(4)]
    qx = jnp.minimum(jnp.minimum(lx[0], lx[1]), jnp.minimum(lx[2], lx[3]))
    qy = jnp.minimum(jnp.minimum(ly[0], ly[1]), jnp.minimum(ly[2], ly[3]))
    at = qx * PAIR + qy * 4
    at = jnp.where(qy == CY, -1 - (2 * EDGE_X + EDGE_Y + 8 * qx), at)
    at = jnp.where(qy == 0, -1 - (2 * EDGE_X + 8 * qx), at)
    at = jnp.where(qx == CX, -1 - (EDGE_X + 4 * qy), at)
    at = jnp.where(qx == 0, -1 - 4 * qy, at)
    flat[...] = jnp.maximum(at, 0)
    rel[0] = 2.0 * (so[0] + (lx[0] - qx).astype(f32))
    rel[1] = 2.0 * (so[1] + (ly[0] - qy).astype(f32))
    rel[2] = 2.0 * so[2]
    for i in range(ROWS // 8):
        p = pix[8 * i : 8 * i + 8, :]
        tile = p >> 8
        low, high = tile & (LANES - 1), tile >> 7
        slot = jnp.zeros((8, LANES), i32)
        for t in range(8):
            row = jnp.broadcast_to(tile_slot[t : t + 1, :], (8, LANES))
            slot = jnp.where(high == t, lane_take(row, low), slot)
        owner[8 * i : 8 * i + 8, :] = slot >> 3
        target[8 * i : 8 * i + 8, :] = (slot & 7) * 256 + (p & 255)
    sub = iota((OWNERS, LANES), 0)
    upper = (iota((LANES, 2 * LANES), 0) <= iota((LANES, 2 * LANES), 1)).astype(f32).astype(bf16)

    def ranks(r, seen):
        hit = sub == jnp.broadcast_to(owner[pl.ds(r, 1), :], (OWNERS, LANES))
        tally = jnp.dot(jnp.where(hit, 1.0, 0.0).astype(bf16), upper, preferred_element_type=f32)
        rank[pl.ds(r, 1), :] = (
            jnp.sum(jnp.where(hit, tally[:, :LANES] + seen, 0.0), axis=0, keepdims=True) - 1.0
        ).astype(i32)
        return seen + tally[:, LANES:]

    lax.fori_loop(0, ROWS, ranks, jnp.zeros((OWNERS, LANES), f32), unroll=32)
    outside = at < 0
    tally = jnp.dot(jnp.where(outside, 1.0, 0.0).astype(bf16), upper, preferred_element_type=f32)
    before = iota((ROWS, ROWS), 1) < iota((ROWS, ROWS), 0)
    ahead = jnp.dot(
        jnp.where(before, 1.0, 0.0).astype(bf16), tally[:, LANES:].astype(bf16), preferred_element_type=f32
    )
    count = (ahead + tally[:, LANES:])[ROWS - 1 :].astype(i32)
    where[0] = jnp.where(outside, (ahead + tally[:, :LANES] - 1.0).astype(i32), -1)
    where[1] = iota((ROWS, LANES), 0) * LANES + iota((ROWS, LANES), 1)
    where[2] = -1 - at
    low_sub = iota((LANES, 2 * LANES), 0)
    high_sub = iota((ROWS, 2 * LANES), 0)

    def collect(r, total):
        spot, point, place = [
            jnp.concatenate([where[k, pl.ds(2 * r, 1), :], where[k, pl.ds(2 * r + 1, 1), :]], axis=1)
            for k in range(3)
        ]
        low_hit = jnp.where(low_sub == (spot & (LANES - 1)), 1.0, 0.0).astype(bf16)
        hit = high_sub == (spot >> 7)
        parts = [(point >> 8), (point & 255), (place >> 8), (place & 255)]
        rows = jnp.concatenate([jnp.where(hit, x.astype(f32), 0.0) for x in parts], axis=0).astype(bf16)
        return total + lax.dot_general(rows, low_hit, NT, preferred_element_type=f32)

    found = lax.fori_loop(0, ROWS // 2, collect, jnp.zeros((4 * ROWS, LANES), f32), unroll=16).astype(i32)
    points[:ROWS] = found[:ROWS] * 256 + found[ROWS : 2 * ROWS]
    places[:ROWS] = found[2 * ROWS : 3 * ROWS] * 256 + found[3 * ROWS :]
    points[ROWS:] = jnp.broadcast_to(count, (8, LANES))
    places[ROWS:] = jnp.broadcast_to(count, (8, LANES))

def inner_kernel(ph, counts, flat, rel, sums, near, table, square, stage_a, stage_b, ssem, *start):
    to_scalar = [pltpu.make_async_copy(flat.at[pl.ds(4 * s, 4)], start[s], ssem.at[s]) for s in range(8)]
    for copy in to_scalar:
        copy.start()
    parts = [[rel[c, pl.ds(v, 8, stride=4), :] for c in range(3)] for v in range(4)]

    def spread(lane, _):
        take = jnp.full((8, LANES), lane, i32)
        for v in range(4):
            for c in range(3):
                near[c, v * LANES + lane] = lane_take(parts[v][c], take)
        return 0

    lax.fori_loop(0, LANES, spread, 0, unroll=32)
    square[:CY, :CX] = counts[...].astype(f32)
    filled = square[:CY, :].astype(i32)
    lane = iota((CY, LANES), 1)

    def row(c, x, y, right):
        return x * PAIR + (c // 2) * TWO + y * 4 + 2 * right + c % 2

    def column(x, _):
        live = lane < lane_take(filled, jnp.full((CY, LANES), x, i32))
        for c in range(6):
            v = ph[c, x]
            v = v + v if c < 3 else jnp.where(live, v, 0.0)
            table[pl.ds(row(c, x + 1, 1, 0), CY, stride=4), :] = v
            table[pl.ds(row(c, x, 1, 1), CY, stride=4), :] = v
        return 0

    lax.fori_loop(0, CX, column, 0, unroll=16)
    for copy in to_scalar:
        copy.wait()
    zero = lax.axis_index("bx") * 0

    def fetch(i, stage):
        for u in range(GROUPS):
            g = jnp.minimum(i * GROUPS + u, POINTS // 8 - 1)
            v, lane = g >> 7, g & (LANES - 1)
            for s in range(8):
                r = start[s][v, lane]
                for j in range(3):
                    stage[u, j, pl.ds(zero + STEP * s, 8), :] = table[pl.ds(r + j * TWO, 8), :]

    def weigh(i, stage):
        for u in range(GROUPS):
            total = weigh_eight(stage.at[u], [near[c, i * GROUPS + u] for c in range(3)])
            for c in range(3):
                sums[c, pl.ds(i * GROUPS + u, 8, stride=APART), :] = total[c]

    def step(i, _):
        weigh(2 * i, stage_a)
        fetch(2 * i + 1, stage_b)
        weigh(2 * i + 1, stage_b)
        fetch(2 * i + 2, stage_a)
        return 0

    fetch(0, stage_a)
    lax.fori_loop(0, POINTS // 16 // GROUPS, step, 0)


def outer_kernel(points, places, sums, near, alb, owner, rank, target, xm, xp, c0, c63, ym, yp, bottom, top,
                 send, edge, stage, close, rad):
    for c in range(6):
        scale = 2.0 if c < 3 else 1.0
        plane = (c // 2) * EDGE + c % 2
        for base, cols in ((0, ((xm, 0), (c0, 1))), (EDGE_X, ((c63, CX), (xp, CX + 1)))):
            for right, (col, x) in enumerate(cols):
                at = plane + base + 2 * right
                edge[pl.ds(at + 4, CY, stride=4), :] = col[c] * scale
                edge[at : at + 1, :] = ym[c, x : x + 1] * scale
                edge[at + 4 * EY - 4 : at + 4 * EY - 3, :] = yp[c, x : x + 1] * scale
        for base, lines in ((2 * EDGE_X, (ym, bottom)), (2 * EDGE_X + EDGE_Y, (top, yp))):
            for yy, line in enumerate(lines):
                for right in range(2):
                    at = plane + base + 4 * yy + 2 * right
                    edge[pl.ds(at, CX + 1, stride=8), :] = line[c, right : right + CX + 1] * scale
    sub = iota((8, LANES), 0)
    zero = lax.axis_index("bx") * 0
    count = points[ROWS, 0]

    def eight(i, stage, close):
        where = []
        for s in range(8):
            k = jnp.minimum(8 * i + s, count - 1)
            p, r = points[k >> 7, k & (LANES - 1)], places[k >> 7, k & (LANES - 1)]
            where.append((p >> 9) * APART + (p & 511))
            for c in range(3):
                close[c, s : s + 1, :] = near[c, p & 511, pl.ds(p >> 9, 1), :]
            for j in range(3):
                stage[j, pl.ds(zero + STEP * s, 8), :] = edge[pl.ds(r + j * EDGE, 8), :]
        total = weigh_eight(stage, [close[c] for c in range(3)])
        for c in range(3):
            for s in range(8):
                sums[c, pl.ds(where[s], 1), :] = total[c][s : s + 1]

    def eights(i, _):
        for u in range(TOGETHER):
            eight(TOGETHER * i + u, stage.at[u], close.at[u])
        return 0

    lax.fori_loop(0, lax.div(count + 8 * TOGETHER - 1, 8 * TOGETHER), eights, 0)
    ones = jnp.ones((8, 2 * LANES), f32).astype(bf16)

    def lane_sums(r, _):
        for c in range(3):
            for k in range(2):
                line = 2 * r + k
                x = sums[c, pl.ds((line >> 2) * APART + (line & 3) * LANES, LANES), :]
                high = x.astype(bf16)
                low = (x - high.astype(f32)).astype(bf16)
                both = jnp.concatenate([high, low], axis=1)
                y = lax.dot_general(ones, both, NT, preferred_element_type=f32)
                rad[c, pl.ds(line, 1), :] = y[:1]
        return 0

    lax.fori_loop(0, ROWS // 2, lane_sums, 0, unroll=16)
    for c in range(3):
        for r in range(ROWS):
            rad[c, r : r + 1, :] = rad[c, r : r + 1, :] * alb[c : c + 1, r * LANES : (r + 1) * LANES]
    wide_sub = iota((OWNERS, 2 * LANES), 0)
    rank_sub = iota((CAP, 2 * LANES), 0)

    def two(ref, r):
        return jnp.concatenate([ref[pl.ds(2 * r, 1), :], ref[pl.ds(2 * r + 1, 1), :]], axis=1)

    def scatter(r, total):
        mine = jnp.where(wide_sub == two(owner, r), 1.0, 0.0).astype(bf16)
        hit = rank_sub == two(rank, r)
        where = two(target, r)
        vals = [two(rad.at[c], r) for c in range(3)]
        high = [x.astype(bf16).astype(f32) for x in vals]
        low = [x - h for x, h in zip(vals, high)]
        high.append((where & ~255).astype(f32))
        low.append((where & 255).astype(f32))
        for part in (high, low):
            rows = jnp.concatenate([jnp.where(hit, x, 0.0) for x in part], axis=0).astype(bf16)
            total = total + lax.dot_general(mine, rows, NT, preferred_element_type=f32)
        return total

    send[:, 0, :] = lax.fori_loop(0, ROWS // 2, scatter, jnp.zeros((OWNERS, 4 * CAP), f32), unroll=16)


def film_kernel(got, film, flipped, total):
    for j in range(3):
        flipped[LANES * j : LANES * j + LANES, :] = jnp.transpose(got[:, 0, LANES * j : LANES * j + LANES])
    lo_sub = iota((LANES, 2 * LANES), 0)
    hi_sub = iota((16, 2 * LANES), 0)

    def two(row):
        return jnp.concatenate(
            [flipped[pl.ds(row, 1), :], flipped[pl.ds(row + CAP // 2, 1), :]], axis=1
        )

    def step(k, acc):
        where = two(3 * CAP + k).astype(i32)
        low_hit = jnp.where(lo_sub == (where & 127), 1.0, 0.0).astype(bf16)
        hit = hi_sub == (where >> 7)
        high, low = [], []
        for c in range(3):
            x = two(c * CAP + k)
            h = x.astype(bf16).astype(f32)
            high.append(jnp.where(hit, h, 0.0))
            low.append(jnp.where(hit, x - h, 0.0))
        rows = jnp.concatenate(high + low, axis=0).astype(bf16)
        return acc + lax.dot_general(rows, low_hit, NT, preferred_element_type=f32)

    acc = lax.fori_loop(0, CAP // 2, step, jnp.zeros((96, LANES), f32), unroll=48)
    total[...] = acc[:48] + acc[48:]
    for c in range(3):
        film[c, :, :LANES] = total[pl.ds(16 * c, 8, stride=2), :]
        film[c, :, LANES:] = total[pl.ds(16 * c + 1, 8, stride=2), :]


def shift(x, axis, by):
    n = lax.axis_size(axis)
    return lax.ppermute(x, axis, [(i, (i + by) % n) for i in range(n)])


def per_device(photon_data, block_counts, gather_offsets, gather_blocks, albedo, gather_pixels, tile_slot):
    small_i = jax.ShapeDtypeStruct((ROWS, LANES), i32)
    listed = jax.ShapeDtypeStruct((LIST, LANES), i32)
    column, line = jax.ShapeDtypeStruct((6, CY, LANES), f32), jax.ShapeDtypeStruct((6, CX, LANES), f32)
    counts = block_counts.T
    c63, c0, top, bottom = pl.pallas_call(
        edge_kernel,
        in_specs=[HBM, VMEM],
        out_specs=[VMEM] * 4,
        out_shape=[column, column, line, line],
        scratch_shapes=[
            pltpu.VMEM((LANES, LANES), f32),
            pltpu.VMEM((2, 6, CY, LANES), f32),
            pltpu.VMEM((2, 6, CX, LANES), f32),
            pltpu.SemaphoreType.DMA((4,)),
        ],
        compiler_params=params(60),
        name="edges",
    )(photon_data, counts)
    xm, xp = shift(c63, "bx", 1), shift(c0, "bx", -1)
    flat, rel, owner, rank, target, points, places = pl.pallas_call(
        prep_kernel,
        in_specs=[VMEM] * 4,
        out_specs=[VMEM] * 7,
        out_shape=[small_i, jax.ShapeDtypeStruct((3, ROWS, LANES), f32), small_i, small_i, small_i, listed, listed],
        scratch_shapes=[
            pltpu.VMEM((4, ROWS, LANES), i32),
            pltpu.VMEM((3, ROWS, LANES), f32),
            pltpu.VMEM((3, ROWS, LANES), i32),
        ],
        compiler_params=params(16),
        cost_estimate=pl.CostEstimate(flops=4000000000, bytes_accessed=40000000, transcendentals=0),
        name="prep",
    )(gather_blocks, gather_offsets, gather_pixels.reshape(ROWS, LANES), tile_slot.reshape(8, LANES))
    top, bottom, rank = lax.optimization_barrier((top, bottom, rank))
    top = jnp.concatenate([xm[:, -1:], top, xp[:, -1:]], axis=1)
    bottom = jnp.concatenate([xm[:, :1], bottom, xp[:, :1]], axis=1)
    ym, yp = shift(top, "by", 1), shift(bottom, "by", -1)
    sums, near = pl.pallas_call(
        inner_kernel,
        in_specs=[VMEM] * 4,
        out_specs=[VMEM] * 2,
        out_shape=[
            jax.ShapeDtypeStruct((3, 8 * APART, LANES), f32),
            jax.ShapeDtypeStruct((3, POINTS // 8, 8, LANES), f32),
        ],
        scratch_shapes=[
            pltpu.VMEM((TABLE_ROWS, LANES), f32),
            pltpu.VMEM((CY, LANES), f32),
            pltpu.VMEM((GROUPS, 3, 8 * STEP + 8, LANES), f32),
            pltpu.VMEM((GROUPS, 3, 8 * STEP + 8, LANES), f32),
            pltpu.SemaphoreType.DMA((8,)),
        ]
        + [pltpu.SMEM((4, LANES), i32)] * 8,
        compiler_params=params(34),
        cost_estimate=pl.CostEstimate(flops=60_000_000, bytes_accessed=7_000_000, transcendentals=0),
        name="inner",
    )(photon_data, counts, flat, rel)
    send = pl.pallas_call(
        outer_kernel,
        in_specs=[SMEM] * 2 + [VMEM] * 14,
        out_specs=VMEM,
        out_shape=jax.ShapeDtypeStruct((OWNERS, 1, 4 * CAP), f32),
        scratch_shapes=[
            pltpu.VMEM((3 * EDGE + 64, LANES), f32),
            pltpu.VMEM((TOGETHER, 3, 8 * STEP + 8, LANES), f32),
            pltpu.VMEM((TOGETHER, 3, 8, LANES), f32),
            pltpu.VMEM((3, ROWS, LANES), f32),
        ],
        compiler_params=params(16),
        name="outer",
    )(points, places, sums, near, albedo, owner, rank, target, xm, xp, c0, c63, ym, yp, bottom, top)
    got = lax.all_to_all(send, AXES, 0, 0, tiled=True)
    return pl.pallas_call(
        film_kernel,
        in_specs=[VMEM],
        out_specs=VMEM,
        out_shape=jax.ShapeDtypeStruct((3, 8, 256), f32),
        scratch_shapes=[pltpu.VMEM((4 * CAP, LANES), f32), pltpu.VMEM((48, LANES), f32)],
        compiler_params=params(16),
        name="film",
    )(got)


def solution(mesh):
    in_specs = (P(None, "bx", "by", None), P("bx", "by"), P(None, AXES), P(None, AXES), P(None, AXES), P(AXES), P())
    return jax.shard_map(per_device, mesh=mesh, in_specs=in_specs, out_specs=P(None, AXES, None), check_vma=False)
```

```python
import jax
import jax.numpy as jnp
from jax import lax
from jax.experimental import pallas as pl
from jax.experimental.pallas import tpu as pltpu
from jax.sharding import PartitionSpec as P

AXES = ("bx", "by")
CX, CY = 64, 32
EX, EY = CX + 2, CY + 2
NXC, NYC = 1024, 256
LANES = 128
POINTS = 4096
ROWS = POINTS // LANES
CAP = 96
OWNERS = 128
TWO = 4 * EY
PAIR = 3 * TWO
TABLE_ROWS = (CX + 1) * PAIR
APART = 513
EDGE_X, EDGE_Y = 4 * EY, 8 * (CX + 1)
EDGE = 2 * EDGE_X + 2 * EDGE_Y
LIST = ROWS + 8
STEP = 9
TOGETHER = 8
GROUPS = 4
i32, f32, bf16 = jnp.int32, jnp.float32, jnp.bfloat16
VMEM = pl.BlockSpec(memory_space=pltpu.VMEM)
SMEM = pl.BlockSpec(memory_space=pltpu.SMEM)
NT = (((1,), (1,)), ((), ()))


HBM = pl.BlockSpec(memory_space=pltpu.HBM)


def params(mib):
    return pltpu.CompilerParams(vmem_limit_bytes=int(mib * 1024 * 1024))


def iota(shape, dim):
    return lax.broadcasted_iota(i32, shape, dim)


def lane_take(x, idx):
    return jnp.take_along_axis(x, idx, axis=1, mode="promise_in_bounds")


def weigh_eight(stage, close):
    far = [x - 2.0 for x in close]
    total = [None] * 3
    for k in range(4):
        yy, xx = k >> 1, k & 1

        def load(c):
            return stage[c // 2, pl.ds(4 * yy + 2 * xx + c % 2, 8, stride=STEP), :]

        o = (far[0] if xx else close[0], far[1] if yy else close[1], close[2])
        d = [load(c) - o[c] for c in range(3)]
        dist = d[0] * d[0] + d[1] * d[1] + d[2] * d[2]
        weight = jnp.maximum(1.0 - dist, 0.0)
        for c in range(3):
            v = weight * load(3 + c)
            total[c] = v if k == 0 else total[c] + v
    return total


def edge_kernel(ph, counts, c63, c0, top, bottom, square, raw_x, raw_y, sem):
    reads = [pltpu.make_async_copy(ph.at[:, x], raw_x.at[k], sem.at[k]) for k, x in enumerate((CX - 1, 0))]
    reads += [pltpu.make_async_copy(ph.at[:, :, y, :], raw_y.at[k], sem.at[2 + k]) for k, y in enumerate((CY - 1, 0))]
    for read in reads:
        read.start()
    square[:CY, :CX] = counts[...].astype(f32)
    by_y = square[:CY, :].astype(i32)
    by_x = jnp.transpose(square[...])[:CX, :].astype(i32)
    for read in reads:
        read.wait()
    for k, (out, x) in enumerate(((c63, CX - 1), (c0, 0))):
        live = iota((CY, LANES), 1) < lane_take(by_y, jnp.full((CY, LANES), x, i32))
        for c in range(6):
            v = raw_x[k, c]
            out[c] = v if c < 3 else jnp.where(live, v, 0.0)
    for k, (out, y) in enumerate(((top, CY - 1), (bottom, 0))):
        live = iota((CX, LANES), 1) < lane_take(by_x, jnp.full((CX, LANES), y, i32))
        for c in range(6):
            v = raw_y[k, c]
            out[c] = v if c < 3 else jnp.where(live, v, 0.0)


def prep_kernel(blocks, offs, pix, tile_slot, flat, rel, owner, rank, target, points, places, sb, so, where):
    for k in range(4):
        for r in range(ROWS):
            sb[k, r : r + 1, :] = blocks[k : k + 1, r * LANES : (r + 1) * LANES]
    for c in range(3):
        for r in range(ROWS):
            so[c, r : r + 1, :] = offs[c : c + 1, r * LANES : (r + 1) * LANES]
    fx, fy = lax.axis_index("bx") * CX, lax.axis_index("by") * CY
    lx = [((sb[k] >> 8) - fx + 1) & (NXC - 1) for k in range(4)]
    ly = [((sb[k] & (NYC - 1)) - fy + 1) & (NYC - 1) for k in range(4)]
    qx = jnp.minimum(jnp.minimum(lx[0], lx[1]), jnp.minimum(lx[2], lx[3]))
    qy = jnp.minimum(jnp.minimum(ly[0], ly[1]), jnp.minimum(ly[2], ly[3]))
    at = qx * PAIR + qy * 4
    at = jnp.where(qy == CY, -1 - (2 * EDGE_X + EDGE_Y + 8 * qx), at)
    at = jnp.where(qy == 0, -1 - (2 * EDGE_X + 8 * qx), at)
    at = jnp.where(qx == CX, -1 - (EDGE_X + 4 * qy), at)
    at = jnp.where(qx == 0, -1 - 4 * qy, at)
    flat[...] = jnp.maximum(at, 0)
    rel[0] = 2.0 * (so[0] + (lx[0] - qx).astype(f32))
    rel[1] = 2.0 * (so[1] + (ly[0] - qy).astype(f32))
    rel[2] = 2.0 * so[2]
    for i in range(ROWS // 8):
        p = pix[8 * i : 8 * i + 8, :]
        tile = p >> 8
        low, high = tile & (LANES - 1), tile >> 7
        slot = jnp.zeros((8, LANES), i32)
        for t in range(8):
            row = jnp.broadcast_to(tile_slot[t : t + 1, :], (8, LANES))
            slot = jnp.where(high == t, lane_take(row, low), slot)
        owner[8 * i : 8 * i + 8, :] = slot >> 3
        target[8 * i : 8 * i + 8, :] = (slot & 7) * 256 + (p & 255)
    sub = iota((OWNERS, LANES), 0)
    upper = (iota((LANES, 2 * LANES), 0) <= iota((LANES, 2 * LANES), 1)).astype(f32).astype(bf16)

    def ranks(r, seen):
        hit = sub == jnp.broadcast_to(owner[pl.ds(r, 1), :], (OWNERS, LANES))
        tally = jnp.dot(jnp.where(hit, 1.0, 0.0).astype(bf16), upper, preferred_element_type=f32)
        rank[pl.ds(r, 1), :] = (
            jnp.sum(jnp.where(hit, tally[:, :LANES] + seen, 0.0), axis=0, keepdims=True) - 1.0
        ).astype(i32)
        return seen + tally[:, LANES:]

    lax.fori_loop(0, ROWS, ranks, jnp.zeros((OWNERS, LANES), f32), unroll=32)
    outside = at < 0
    tally = jnp.dot(jnp.where(outside, 1.0, 0.0).astype(bf16), upper, preferred_element_type=f32)
    before = iota((ROWS, ROWS), 1) < iota((ROWS, ROWS), 0)
    ahead = jnp.dot(
        jnp.where(before, 1.0, 0.0).astype(bf16), tally[:, LANES:].astype(bf16), preferred_element_type=f32
    )
    count = (ahead + tally[:, LANES:])[ROWS - 1 :].astype(i32)
    where[0] = jnp.where(outside, (ahead + tally[:, :LANES] - 1.0).astype(i32), -1)
    where[1] = iota((ROWS, LANES), 0) * LANES + iota((ROWS, LANES), 1)
    where[2] = -1 - at
    low_sub = iota((LANES, 2 * LANES), 0)
    high_sub = iota((ROWS, 2 * LANES), 0)

    def collect(r, total):
        spot, point, place = [
            jnp.concatenate([where[k, pl.ds(2 * r, 1), :], where[k, pl.ds(2 * r + 1, 1), :]], axis=1)
            for k in range(3)
        ]
        low_hit = jnp.where(low_sub == (spot & (LANES - 1)), 1.0, 0.0).astype(bf16)
        hit = high_sub == (spot >> 7)
        parts = [(point >> 8), (point & 255), (place >> 8), (place & 255)]
        rows = jnp.concatenate([jnp.where(hit, x.astype(f32), 0.0) for x in parts], axis=0).astype(bf16)
        return total + lax.dot_general(rows, low_hit, NT, preferred_element_type=f32)

    found = lax.fori_loop(0, ROWS // 2, collect, jnp.zeros((4 * ROWS, LANES), f32), unroll=16).astype(i32)
    points[:ROWS] = found[:ROWS] * 256 + found[ROWS : 2 * ROWS]
    places[:ROWS] = found[2 * ROWS : 3 * ROWS] * 256 + found[3 * ROWS :]
    points[ROWS:] = jnp.broadcast_to(count, (8, LANES))
    places[ROWS:] = jnp.broadcast_to(count, (8, LANES))

def inner_kernel(ph, counts, flat, rel, sums, near, table, square, stage_a, stage_b, ssem, *start):
    to_scalar = [pltpu.make_async_copy(flat.at[pl.ds(4 * s, 4)], start[s], ssem.at[s]) for s in range(8)]
    for copy in to_scalar:
        copy.start()
    parts = [[rel[c, pl.ds(v, 8, stride=4), :] for c in range(3)] for v in range(4)]

    def spread(lane, _):
        take = jnp.full((8, LANES), lane, i32)
        for v in range(4):
            for c in range(3):
                near[c, v * LANES + lane] = lane_take(parts[v][c], take)
        return 0

    lax.fori_loop(0, LANES, spread, 0, unroll=32)
    square[:CY, :CX] = counts[...].astype(f32)
    filled = square[:CY, :].astype(i32)
    lane = iota((CY, LANES), 1)

    def row(c, x, y, right):
        return x * PAIR + (c // 2) * TWO + y * 4 + 2 * right + c % 2

    def column(x, _):
        live = lane < lane_take(filled, jnp.full((CY, LANES), x, i32))
        for c in range(6):
            v = ph[c, x]
            v = v + v if c < 3 else jnp.where(live, v, 0.0)
            table[pl.ds(row(c, x + 1, 1, 0), CY, stride=4), :] = v
            table[pl.ds(row(c, x, 1, 1), CY, stride=4), :] = v
        return 0

    lax.fori_loop(0, CX, column, 0, unroll=16)
    for copy in to_scalar:
        copy.wait()
    zero = lax.axis_index("bx") * 0

    def fetch(i, stage):
        for u in range(GROUPS):
            g = jnp.minimum(i * GROUPS + u, POINTS // 8 - 1)
            v, lane = g >> 7, g & (LANES - 1)
            for s in range(8):
                r = start[s][v, lane]
                for j in range(3):
                    stage[u, j, pl.ds(zero + STEP * s, 8), :] = table[pl.ds(r + j * TWO, 8), :]

    def weigh(i, stage):
        for u in range(GROUPS):
            total = weigh_eight(stage.at[u], [near[c, i * GROUPS + u] for c in range(3)])
            for c in range(3):
                sums[c, pl.ds(i * GROUPS + u, 8, stride=APART), :] = total[c]

    def step(i, _):
        weigh(2 * i, stage_a)
        fetch(2 * i + 1, stage_b)
        weigh(2 * i + 1, stage_b)
        fetch(2 * i + 2, stage_a)
        return 0

    fetch(0, stage_a)
    lax.fori_loop(0, POINTS // 16 // GROUPS, step, 0)


def outer_kernel(points, places, sums, near, alb, owner, rank, target, xm, xp, c0, c63, ym, yp, bottom, top,
                 send, edge, stage, close, rad):
    for c in range(6):
        scale = 2.0 if c < 3 else 1.0
        plane = (c // 2) * EDGE + c % 2
        for base, lines in ((2 * EDGE_X + EDGE_Y, (top, yp)), (2 * EDGE_X, (ym, bottom))):
            for yy, line in enumerate(lines):
                at = plane + base + 4 * yy
                value = line[c] * scale
                edge[pl.ds(at - 6, CX + 2, stride=8), :] = value
                edge[pl.ds(at, CX + 1, stride=8), :] = value[: CX + 1]
        for base, cols in ((0, ((xm, 0), (c0, 1))), (EDGE_X, ((c63, CX), (xp, CX + 1)))):
            for right, (col, x) in enumerate(cols):
                at = plane + base + 2 * right
                edge[pl.ds(at + 4, CY, stride=4), :] = col[c] * scale
                edge[at : at + 1, :] = ym[c, x : x + 1] * scale
                edge[at + 4 * EY - 4 : at + 4 * EY - 3, :] = yp[c, x : x + 1] * scale
    sub = iota((8, LANES), 0)
    zero = lax.axis_index("bx") * 0
    count = points[ROWS, 0]

    def eight(i, stage, close):
        where = []
        for s in range(8):
            k = jnp.minimum(8 * i + s, count - 1)
            p, r = points[k >> 7, k & (LANES - 1)], places[k >> 7, k & (LANES - 1)]
            where.append((p >> 9) * APART + (p & 511))
            for c in range(3):
                close[c, s : s + 1, :] = near[c, p & 511, pl.ds(p >> 9, 1), :]
            for j in range(3):
                stage[j, pl.ds(zero + STEP * s, 8), :] = edge[pl.ds(r + j * EDGE, 8), :]
        total = weigh_eight(stage, [close[c] for c in range(3)])
        for c in range(3):
            for s in range(8):
                sums[c, pl.ds(where[s], 1), :] = total[c][s : s + 1]

    def eights(i, _):
        for u in range(TOGETHER):
            eight(TOGETHER * i + u, stage.at[u], close.at[u])
        return 0

    lax.fori_loop(0, lax.div(count + 8 * TOGETHER - 1, 8 * TOGETHER), eights, 0)
    ones = jnp.ones((8, 2 * LANES), f32).astype(bf16)

    def lane_sums(r, _):
        for c in range(3):
            for k in range(2):
                line = 2 * r + k
                x = sums[c, pl.ds((line >> 2) * APART + (line & 3) * LANES, LANES), :]
                high = x.astype(bf16)
                low = (x - high.astype(f32)).astype(bf16)
                both = jnp.concatenate([high, low], axis=1)
                y = lax.dot_general(ones, both, NT, preferred_element_type=f32)
                rad[c, pl.ds(line, 1), :] = y[:1]
        return 0

    lax.fori_loop(0, ROWS // 2, lane_sums, 0, unroll=16)
    for c in range(3):
        for r in range(ROWS):
            rad[c, r : r + 1, :] = rad[c, r : r + 1, :] * alb[c : c + 1, r * LANES : (r + 1) * LANES]
    wide_sub = iota((OWNERS, 2 * LANES), 0)
    rank_sub = iota((CAP, 2 * LANES), 0)

    def two(ref, r):
        return jnp.concatenate([ref[pl.ds(2 * r, 1), :], ref[pl.ds(2 * r + 1, 1), :]], axis=1)

    def scatter(r, total):
        mine = jnp.where(wide_sub == two(owner, r), 1.0, 0.0).astype(bf16)
        hit = rank_sub == two(rank, r)
        where = two(target, r)
        vals = [two(rad.at[c], r) for c in range(3)]
        high = [x.astype(bf16).astype(f32) for x in vals]
        low = [x - h for x, h in zip(vals, high)]
        high.append((where & ~255).astype(f32))
        low.append((where & 255).astype(f32))
        for part in (high, low):
            rows = jnp.concatenate([jnp.where(hit, x, 0.0) for x in part], axis=0).astype(bf16)
            total = total + lax.dot_general(mine, rows, NT, preferred_element_type=f32)
        return total

    send[:, 0, :] = lax.fori_loop(0, ROWS // 2, scatter, jnp.zeros((OWNERS, 4 * CAP), f32), unroll=16)


def film_kernel(got, film, flipped, total):
    for j in range(3):
        flipped[LANES * j : LANES * j + LANES, :] = jnp.transpose(got[:, 0, LANES * j : LANES * j + LANES])
    lo_sub = iota((LANES, 2 * LANES), 0)
    hi_sub = iota((16, 2 * LANES), 0)

    def two(row):
        return jnp.concatenate(
            [flipped[pl.ds(row, 1), :], flipped[pl.ds(row + CAP // 2, 1), :]], axis=1
        )

    def step(k, acc):
        where = two(3 * CAP + k).astype(i32)
        low_hit = jnp.where(lo_sub == (where & 127), 1.0, 0.0).astype(bf16)
        hit = hi_sub == (where >> 7)
        high, low = [], []
        for c in range(3):
            x = two(c * CAP + k)
            h = x.astype(bf16).astype(f32)
            high.append(jnp.where(hit, h, 0.0))
            low.append(jnp.where(hit, x - h, 0.0))
        rows = jnp.concatenate(high + low, axis=0).astype(bf16)
        return acc + lax.dot_general(rows, low_hit, NT, preferred_element_type=f32)

    acc = lax.fori_loop(0, CAP // 2, step, jnp.zeros((96, LANES), f32), unroll=48)
    total[...] = acc[:48] + acc[48:]
    for c in range(3):
        film[c, :, :LANES] = total[pl.ds(16 * c, 8, stride=2), :]
        film[c, :, LANES:] = total[pl.ds(16 * c + 1, 8, stride=2), :]


def shift(x, axis, by):
    n = lax.axis_size(axis)
    return lax.ppermute(x, axis, [(i, (i + by) % n) for i in range(n)])


def per_device(photon_data, block_counts, gather_offsets, gather_blocks, albedo, gather_pixels, tile_slot):
    small_i = jax.ShapeDtypeStruct((ROWS, LANES), i32)
    listed = jax.ShapeDtypeStruct((LIST, LANES), i32)
    column, line = jax.ShapeDtypeStruct((6, CY, LANES), f32), jax.ShapeDtypeStruct((6, CX, LANES), f32)
    counts = block_counts.T
    c63, c0, top, bottom = pl.pallas_call(
        edge_kernel,
        in_specs=[HBM, VMEM],
        out_specs=[VMEM] * 4,
        out_shape=[column, column, line, line],
        scratch_shapes=[
            pltpu.VMEM((LANES, LANES), f32),
            pltpu.VMEM((2, 6, CY, LANES), f32),
            pltpu.VMEM((2, 6, CX, LANES), f32),
            pltpu.SemaphoreType.DMA((4,)),
        ],
        compiler_params=params(60),
        name="edges",
    )(photon_data, counts)
    xm, xp = shift(c63, "bx", 1), shift(c0, "bx", -1)
    flat, rel, owner, rank, target, points, places = pl.pallas_call(
        prep_kernel,
        in_specs=[VMEM] * 4,
        out_specs=[VMEM] * 7,
        out_shape=[small_i, jax.ShapeDtypeStruct((3, ROWS, LANES), f32), small_i, small_i, small_i, listed, listed],
        scratch_shapes=[
            pltpu.VMEM((4, ROWS, LANES), i32),
            pltpu.VMEM((3, ROWS, LANES), f32),
            pltpu.VMEM((3, ROWS, LANES), i32),
        ],
        compiler_params=params(16),
        cost_estimate=pl.CostEstimate(flops=4000000000, bytes_accessed=40000000, transcendentals=0),
        name="prep",
    )(gather_blocks, gather_offsets, gather_pixels.reshape(ROWS, LANES), tile_slot.reshape(8, LANES))
    top, bottom, rank = lax.optimization_barrier((top, bottom, rank))
    top = jnp.concatenate([xm[:, -1:], top, xp[:, -1:]], axis=1)
    bottom = jnp.concatenate([xm[:, :1], bottom, xp[:, :1]], axis=1)
    ym, yp = shift(top, "by", 1), shift(bottom, "by", -1)
    sums, near = pl.pallas_call(
        inner_kernel,
        in_specs=[VMEM] * 4,
        out_specs=[VMEM] * 2,
        out_shape=[
            jax.ShapeDtypeStruct((3, 8 * APART, LANES), f32),
            jax.ShapeDtypeStruct((3, POINTS // 8, 8, LANES), f32),
        ],
        scratch_shapes=[
            pltpu.VMEM((TABLE_ROWS, LANES), f32),
            pltpu.VMEM((CY, LANES), f32),
            pltpu.VMEM((GROUPS, 3, 8 * STEP + 8, LANES), f32),
            pltpu.VMEM((GROUPS, 3, 8 * STEP + 8, LANES), f32),
            pltpu.SemaphoreType.DMA((8,)),
        ]
        + [pltpu.SMEM((4, LANES), i32)] * 8,
        compiler_params=params(34),
        cost_estimate=pl.CostEstimate(flops=60_000_000, bytes_accessed=7_000_000, transcendentals=0),
        name="inner",
    )(photon_data, counts, flat, rel)
    send = pl.pallas_call(
        outer_kernel,
        in_specs=[SMEM] * 2 + [VMEM] * 14,
        out_specs=VMEM,
        out_shape=jax.ShapeDtypeStruct((OWNERS, 1, 4 * CAP), f32),
        scratch_shapes=[
            pltpu.VMEM((3 * EDGE + 64, LANES), f32),
            pltpu.VMEM((TOGETHER, 3, 8 * STEP + 8, LANES), f32),
            pltpu.VMEM((TOGETHER, 3, 8, LANES), f32),
            pltpu.VMEM((3, ROWS, LANES), f32),
        ],
        compiler_params=params(16),
        name="outer",
    )(points, places, sums, near, albedo, owner, rank, target, xm, xp, c0, c63, ym, yp, bottom, top)
    got = lax.all_to_all(send, AXES, 0, 0, tiled=True)
    return pl.pallas_call(
        film_kernel,
        in_specs=[VMEM],
        out_specs=VMEM,
        out_shape=jax.ShapeDtypeStruct((3, 8, 256), f32),
        scratch_shapes=[pltpu.VMEM((4 * CAP, LANES), f32), pltpu.VMEM((48, LANES), f32)],
        compiler_params=params(16),
        name="film",
    )(got)


def solution(mesh):
    in_specs = (P(None, "bx", "by", None), P("bx", "by"), P(None, AXES), P(None, AXES), P(None, AXES), P(AXES), P())
    return jax.shard_map(per_device, mesh=mesh, in_specs=in_specs, out_specs=P(None, AXES, None), check_vma=False)
```
